256 devices in a mesh: group: 2 (over y), station: 16 (over z), tm: 4 (over x), chan: 2 (over core).
Axes of the slice: x: 4, y: 2, z: 16, core: 2. Of those that a mesh axis runs over, the one named last changes fastest.
The devices are a block of a 4x16x16 slice.
Arguments:
- voltages: bfloat16 [32, 128, 2, 96, 512], P(('group', 'station'), 'chan', None, None, 'tm'), parts along dimension 0, may hold values from -6 to 6
- delays: int32 [32], P(('group', 'station')), parts along dimension 0, may hold values from 0 to 16, as said below
- tap_sets: int32 [32, 128], P(('group', 'station'), 'chan'), parts along dimension 0, may hold values from 0 to 15
- tap_table: bfloat16 [16, 16], replicated, may hold values from -1.5 to 1.5
- weights: bfloat16 [32, 128, 2, 96, 128], P(('group', 'station'), 'chan'), parts along dimension 0, may hold values from -0.15625 to 0.15625
Outputs:
- array_beams: bfloat16 [256, 2, 128, 512], P(('group', 'chan', 'station'), None, None, 'tm'), parts along dimension 0
The draws below stay inside these ranges and needn't reach their ends.
There are 2 independent parts, one for each index of `group`. The reference program is written for one: setup_inputs(seed, part) draws one part's arguments, and reference() takes and returns one part's arrays. A program takes and returns all parts, laid end to end along the dimension named above; an argument that names none is the same for every part. Nothing has to cross between parts.
Inputs may be any that keep to these rules, and one draw needn't show every extreme that they name: `delays`: every delay lies in 0 to 16, and some station has delay 16.
All inputs are finite; a program needn't handle non-finite values.
Results may differ from the reference program's by a relative error of at most 0.0049.
Values may be sent and summed in bfloat16 or wider, within the bound.
A program may use at most 64 MiB of HBM per device.

```python
import jax
import jax.numpy as jnp
from jax import lax

ANTENNA_COUNT = 96
BEAM_TOTAL = 128
TAPS = 16
MAXD = 16
NSETS = 16
STATION_TOTAL = 16
FREQUENCY_BINS = 128
TIME_SAMPLES = 512


def draw_delays(key, part):
    drawn = jax.random.randint(key, (STATION_TOTAL,), 0, MAXD + 1)
    chosen = jax.random.randint(jax.random.fold_in(key, 7), (), 0, STATION_TOTAL)
    positions = jnp.arange(STATION_TOTAL)
    return jnp.where(positions == chosen, MAXD, drawn).astype(jnp.int32)


def plant(array, own_key, least, largest):
    longest = array.shape.index(max(array.shape))
    spots = []
    for shift in (0, 1):
        where = [jax.random.randint(jax.random.fold_in(own_key, axis), (), 0, length) for axis, length in enumerate(array.shape)]
        where[longest] = (where[longest] + shift) % array.shape[longest]
        spots.append(tuple(where))
    return array.at[spots[0]].set(least).at[spots[1]].set(largest)


def raised(values, key, source, target, shards_of, factor):
    def block_of(axis_at):
        return (jnp.arange(values.shape[axis_at]) // (values.shape[axis_at] // shards_of)).reshape((-1,) + (1,) * (values.ndim - 1 - axis_at))

    near = jax.random.permutation(key, shards_of)[block_of(target)]
    other_side = (block_of(target) + shards_of // 2) % shards_of
    return jnp.where((block_of(source) == near) | (block_of(source) == other_side), factor * values, values)


def levels(key, dims, cuts, low, top_value):
    def one(dim, parts):
        heights = jax.random.uniform(jax.random.fold_in(jax.random.fold_in(key, 6), dim), (parts,), jnp.float32, low / len(cuts), top_value / len(cuts))
        return jnp.repeat(jnp.exp(heights), dims[dim] // parts).reshape((-1,) + (1,) * (len(dims) - dim - 1))

    level = one(*cuts[0])
    for cut in cuts[1:]:
        level = level * one(*cut)
    return level


def gaussian(own_key, dims, width, reach, pieces=(), dtype=jnp.bfloat16):
    loudness = levels(own_key, dims, pieces, -0.22, 0.18) if pieces else 1.0
    array = jax.random.normal(own_key, dims, jnp.float32) * width * loudness
    return jnp.minimum(jnp.maximum(array, -reach), reach).astype(dtype)


def bell_draw_with(key, shape, spread, reach, split, heavy, held_as=jnp.bfloat16):
    values = spread * jax.random.normal(key, shape, jnp.float32)
    if split:
        values = values * levels(key, shape, split, -0.22, 0.18)
    return jnp.clip(raised(values, jax.random.fold_in(key, 3), *heavy), -reach, reach).astype(held_as)


def setup_inputs(seed: int = 0, part: int = 0) -> dict:
    key_of = jax.random.split(jax.random.key(seed), 6)
    part_splits = jax.random.split(jax.random.fold_in(key_of[5], part), 6)
    voltages = gaussian(part_splits[0], (STATION_TOTAL, FREQUENCY_BINS, 2, ANTENNA_COUNT, TIME_SAMPLES), 1.0, 6.0, ((0, 16), (1, 2), (4, 4)))
    delays = draw_delays(jax.random.fold_in(jax.random.fold_in(key_of[5], part), 71), part)
    tap_sets = plant(jax.random.randint(part_splits[2], (STATION_TOTAL, FREQUENCY_BINS), 0, NSETS), jax.random.fold_in(part_splits[2], 1), 0, NSETS - 1).astype(jnp.int32)
    tap_table = gaussian(key_of[3], (NSETS, TAPS), 0.25, 1.5)
    weights = bell_draw_with(part_splits[4], (STATION_TOTAL, FREQUENCY_BINS, 2, ANTENNA_COUNT, BEAM_TOTAL), (2 * ANTENNA_COUNT * STATION_TOTAL) ** -0.5, 0.15625, ((0, 16), (1, 2)), (0, 1, 16, 2.0))
    return {"voltages": voltages, "delays": delays, "tap_sets": tap_sets, "tap_table": tap_table, "weights": weights}


def reference(voltages, delays, tap_sets, tap_table, weights):
    halo_len = MAXD + TAPS - 1
    table_f32 = tap_table.astype(jnp.float32)

    def one_station(running, station_item):
        samples, delay_now, chosen_sets, steer = station_item
        samples_f32 = samples.astype(jnp.float32)
        padded = jnp.pad(samples_f32, ((0, 0), (0, 0), (0, 0), (halo_len, 0)))
        coefficients = table_f32[chosen_sets]
        summed_taps = jnp.zeros(samples_f32.shape, jnp.float32)
        for tap_index in range(TAPS):
            begin = (halo_len - delay_now - tap_index).astype(jnp.int32)
            shifted = lax.dynamic_slice_in_dim(padded, begin, TIME_SAMPLES, 3)
            summed_taps = summed_taps + coefficients[:, tap_index][:, None, None, None] * shifted
        delayed_voltages = lax.optimization_barrier(summed_taps.astype(jnp.bfloat16)).astype(jnp.float32)
        steer_f32 = steer.astype(jnp.float32)
        real_in = delayed_voltages[:, 0]
        imag_in = delayed_voltages[:, 1]
        real_part = jnp.einsum('cat,cab->cbt', real_in, steer_f32[:, 0]) - jnp.einsum('cat,cab->cbt', imag_in, steer_f32[:, 1])
        imag_part = jnp.einsum('cat,cab->cbt', real_in, steer_f32[:, 1]) + jnp.einsum('cat,cab->cbt', imag_in, steer_f32[:, 0])
        return running + jnp.stack([real_part, imag_part], axis=1), None

    start_sum = jnp.zeros((FREQUENCY_BINS, 2, BEAM_TOTAL, TIME_SAMPLES), jnp.float32)
    result, unused = lax.scan(one_station, start_sum, (voltages, delays, tap_sets, weights))
    return result.astype(jnp.bfloat16)
```

```python
import functools

import jax
import jax.numpy as jnp
from jax import lax
from jax.experimental import pallas as pl
from jax.experimental.pallas import tpu as pltpu
from jax.sharding import PartitionSpec as P

TAPS = 16
MAXD = 16
RIM = 32
MESH = pl.DeviceIdType.MESH
F32 = jnp.float32
BF16 = jnp.bfloat16


def dot_nt(left, right):
    return lax.dot_general(left, right, (((1,), (1,)), ((), ())), preferred_element_type=F32)


def kernel(
    ring,
    blocks,
    volt,
    steer,
    sets_hbm,
    delays,
    taps_hbm,
    out,
    sets,
    taps,
    vbuf,
    wbuf,
    rim_out,
    rim_in,
    band,
    band_rim,
    top,
    own,
    send,
    recv,
    small_sem,
    load_sem,
    rim_send,
    rim_recv,
    ring_send,
    ring_recv,
):
    me = lax.axis_index("station")
    block = lax.axis_index("tm")
    middle = ring // 2
    per = vbuf.shape[1]
    time = vbuf.shape[3]
    rows = vbuf.shape[2]
    antennas = rows // 2
    set_count = taps.shape[0]
    sides = (lax.rem(me + 1, ring), lax.rem(me + ring - 1, ring))

    barrier = pltpu.get_barrier_semaphore()
    for side in sides:
        pl.semaphore_signal(barrier, inc=1, device_id={"station": side}, device_id_type=MESH)

    @pl.when(block > 0)
    def _():
        pl.semaphore_signal(barrier, inc=1, device_id={"tm": block - 1}, device_id_type=MESH)

    @pl.when(block < blocks - 1)
    def _():
        pl.semaphore_signal(barrier, inc=1, device_id={"tm": block + 1}, device_id_type=MESH)

    def block_of(slot):
        odd = slot % 2
        distance = jnp.where(odd == 1, ring - (slot + 1) // 2, slot // 2)
        return lax.rem(me + middle + distance, ring)

    def load(slot, which):
        source, target = ((volt, vbuf), (steer, wbuf))[which]
        at = block_of(slot) * per
        return pltpu.make_async_copy(source.at[pl.ds(at, per)], target.at[slot], load_sem.at[slot, which])

    def start_loads(slot):
        load(slot, 0).start()
        load(slot, 1).start()

    small = [
        pltpu.make_async_copy(source, target, small_sem.at[index])
        for index, (source, target) in enumerate(((taps_hbm, taps), (sets_hbm, sets)))
    ]
    for copy in small:
        copy.start()
    for slot in range(3):
        start_loads(slot)
    for copy in small:
        copy.wait()

    delay = delays[0]
    table = taps[...].astype(F32)
    lane = lax.broadcasted_iota(jnp.int32, (set_count, time), 1)
    base = jnp.zeros((set_count, time), F32)
    for tap in range(TAPS):
        base = jnp.where((lane + (tap + delay)) % time == 0, table[:, tap : tap + 1], base)
    row_at = lax.broadcasted_iota(jnp.int32, (time, time), 0)
    col_at = lax.broadcasted_iota(jnp.int32, (time, time), 1)
    for index in range(set_count):
        spread = jnp.broadcast_to(base[index : index + 1], (time, time))
        turned = pltpu.roll(spread, 0, 1, stride=1, stride_axis=0)
        band[index] = jnp.where(col_at <= row_at, turned, 0.0).astype(BF16)
        turned = pltpu.roll(spread[:RIM], RIM, 1, stride=1, stride_axis=0)
        band_rim[index] = turned[:, :RIM].astype(BF16)

    pick_row = lax.broadcasted_iota(jnp.int32, (RIM, time), 0)
    pick_col = lax.broadcasted_iota(jnp.int32, (RIM, time), 1)
    pick = jnp.where(pick_col == pick_row + (time - RIM), 1.0, 0.0).astype(BF16)

    def rim_copy(slot):
        return pltpu.make_async_remote_copy(
            src_ref=rim_out.at[slot],
            dst_ref=rim_in.at[slot],
            send_sem=rim_send.at[slot],
            recv_sem=rim_recv.at[slot],
            device_id={"tm": lax.rem(block + 1, blocks)},
            device_id_type=MESH,
        )

    def send_rim(slot):
        @pl.when(block < blocks - 1)
        def _():
            for ch in range(per):
                rim_out[slot, ch] = dot_nt(pick, vbuf[slot, ch]).astype(BF16)
            rim_copy(slot).start()

    def wait_rim(slot):
        @pl.when(block > 0)
        def _():
            rim_copy(slot).wait_recv()

    @pl.when(block == 0)
    def _():
        rim_in[...] = jnp.zeros_like(rim_in)

    def steering(slot, ch):
        real_w = wbuf[slot, ch, :antennas]
        imag_w = wbuf[slot, ch, antennas:]
        upper = jnp.concatenate([real_w, imag_w], axis=1)
        lower = jnp.concatenate([-imag_w, real_w], axis=1)
        return jnp.concatenate([upper, lower], axis=0)

    def filtered(slot, ch):
        chosen = sets[0, block_of(slot) * per + ch]
        return chosen, dot_nt(band[chosen], vbuf[slot, ch])

    def with_rim(slot, ch, chosen, early):
        return early + jnp.dot(band_rim[chosen], rim_in[slot, ch], preferred_element_type=F32)

    def beams(slot, ch):
        chosen, full = filtered(slot, ch)
        early = with_rim(slot, ch, chosen, full[:RIM])
        delayed = jnp.concatenate([early, full[RIM:]], axis=0).astype(BF16)
        return jnp.dot(delayed, steering(slot, ch), preferred_element_type=F32)

    def ring_copy(way, step, ch, part=None):
        span = pl.ds(0, time) if part is None else part
        return pltpu.make_async_remote_copy(
            src_ref=send.at[way, step, ch, span],
            dst_ref=recv.at[way, step, ch, span],
            send_sem=ring_send.at[way, step, ch],
            recv_sem=ring_recv.at[way, step, ch],
            device_id={"station": sides[way]},
            device_id_type=MESH,
        )

    half = per // 2
    order = ([(q + half) % per for q in range(per)], list(range(per)))
    first_way = [0 if ch < half else 1 for ch in range(per)]

    load(0, 0).wait()
    greeters = 2 + jnp.where(block > 0, 1, 0) + jnp.where(block < blocks - 1, 1, 0)
    pl.semaphore_wait(barrier, greeters)
    send_rim(0)
    for slot in range(3, ring):
        start_loads(slot)
    load(0, 1).wait()
    early_span, late_span = pl.ds(0, RIM), pl.ds(RIM, time - RIM)
    for q in range(half):
        for ch in (q, q + half):
            way = first_way[ch]
            chosen, full = filtered(0, ch)
            top[ch] = full[:RIM]
            late = jnp.dot(full[RIM:].astype(BF16), steering(0, ch), preferred_element_type=F32)
            send[way, 0, ch, RIM:] = late.astype(BF16)
            ring_copy(way, 0, ch, late_span).start()
    for slot in (1, 2):
        load(slot, 0).wait()
        send_rim(slot)
    wait_rim(0)
    for q in range(half):
        for ch in (q, q + half):
            way = first_way[ch]
            early = with_rim(0, ch, sets[0, block_of(0) * per + ch], top[ch]).astype(BF16)
            early = jnp.dot(early, steering(0, ch), preferred_element_type=F32)
            send[way, 0, ch, :RIM] = early.astype(BF16)
            ring_copy(way, 0, ch, early_span).start()
    for slot in (1, 2):
        load(slot, 1).wait()
        wait_rim(slot)
    for q in range(per):
        for way in (0, 1):
            own[1, way, order[way][q]] = beams(1 + way, order[way][q])
    for slot in (3, 4):
        if slot < ring:
            load(slot, 0).wait()
            send_rim(slot)

    def one_step(step, first, last):
        now, later = step % 2, (step + 1) % 2
        coming = (2 * step + 1,) if last else (2 * step + 1, 2 * step + 2)
        for q in range(per):
            for way in (0, 1):
                ch = order[way][q]
                total = own[now, way, ch]
                if not first or q >= half:
                    ring_copy(way, step - 1, ch).wait_recv()
                    total = total + recv[way, step - 1, ch].astype(F32)
                send[way, step, ch] = total.astype(BF16)
                ring_copy(way, step, ch).start()
            if q == 0:
                for slot in coming:
                    load(slot, 1).wait()
                    wait_rim(slot)
            for way, slot in enumerate(coming):
                ch = order[way][q]
                own[later, way, ch] = beams(slot, ch)

    def prepare(slots):
        for slot in slots:
            load(slot, 0).wait()
            send_rim(slot)

    for step in range(1, middle):
        if 2 <= step < middle - 2:
            continue
        if step == middle - 2 and middle - 2 > 2:

            @pl.loop(2, middle - 2)
            def _(at):
                one_step(at, False, False)
                prepare((2 * at + 3, 2 * at + 4))

        one_step(step, step == 1, step == middle - 1)
        if step + 2 < middle:
            prepare((2 * step + 3, 2 * step + 4))
        elif step + 2 == middle:
            prepare((2 * step + 3,))

    end = middle % 2
    for q in range(per):
        for way in (0, 1):
            ch = order[way][q]
            ring_copy(way, middle - 1, ch).wait_recv()
            total = own[end, 0, ch] + recv[way, middle - 1, ch].astype(F32)
            if q < half:
                own[end, 0, ch] = total
            else:
                out[ch] = total.T.astype(BF16)

    for ch in range(per):
        ring_copy(first_way[ch], 0, ch).wait_send()

    @pl.loop(1, middle)
    def _(at):
        for way in (0, 1):
            for ch in range(per):
                ring_copy(way, at, ch).wait_send()

    @pl.when(block < blocks - 1)
    def _():
        @pl.loop(0, ring)
        def _(slot):
            rim_copy(slot).wait_send()


def body(ring, blocks, voltages, delays, tap_sets, tap_table, weights):
    _, channels, parts, antennas, time = voltages.shape
    beams = weights.shape[-1]
    per = channels // ring
    rows = parts * antennas
    middle = ring // 2
    set_count = tap_table.shape[0]
    out = pl.pallas_call(
        functools.partial(kernel, ring, blocks),
        out_shape=jax.ShapeDtypeStruct((per, 2 * beams, time), BF16),
        in_specs=[
            pl.BlockSpec(memory_space=pltpu.HBM),
            pl.BlockSpec(memory_space=pltpu.HBM),
            pl.BlockSpec(memory_space=pltpu.HBM),
            pl.BlockSpec(memory_space=pltpu.SMEM),
            pl.BlockSpec(memory_space=pltpu.HBM),
        ],
        out_specs=pl.BlockSpec(memory_space=pltpu.VMEM),
        scratch_shapes=[
            pltpu.SMEM(tap_sets.shape, jnp.int32),
            pltpu.VMEM(tap_table.shape, BF16),
            pltpu.VMEM((ring, per, rows, time), BF16),
            pltpu.VMEM((ring, per, rows, beams), BF16),
            pltpu.VMEM((ring, per, RIM, rows), BF16),
            pltpu.VMEM((ring, per, RIM, rows), BF16),
            pltpu.VMEM((set_count, time, time), BF16),
            pltpu.VMEM((set_count, RIM, RIM), BF16),
            pltpu.VMEM((per, RIM, rows), F32),
            pltpu.VMEM((2, 2, per, time, 2 * beams), F32),
            pltpu.VMEM((2, middle, per, time, 2 * beams), BF16),
            pltpu.VMEM((2, middle, per, time, 2 * beams), BF16),
            pltpu.SemaphoreType.DMA((2,)),
            pltpu.SemaphoreType.DMA((ring, 2)),
            pltpu.SemaphoreType.DMA((ring,)),
            pltpu.SemaphoreType.DMA((ring,)),
            pltpu.SemaphoreType.DMA((2, middle, per)),
            pltpu.SemaphoreType.DMA((2, middle, per)),
        ],
        compiler_params=pltpu.CompilerParams(
            collective_id=0, has_side_effects=True, vmem_limit_bytes=63 * 1024 * 1024
        ),
    )(
        voltages.reshape(channels, rows, time),
        weights.reshape(channels, rows, beams),
        tap_sets,
        delays,
        tap_table,
    )
    return out.reshape(per, 2, beams, time)


def solution(mesh):
    return jax.shard_map(
        functools.partial(body, mesh.shape["station"], mesh.shape["tm"]),
        mesh=mesh,
        in_specs=(
            P(("group", "station"), "chan", None, None, "tm"),
            P(("group", "station")),
            P(("group", "station"), "chan"),
            P(),
            P(("group", "station"), "chan", None, None, None),
        ),
        out_specs=P(("group", "chan", "station"), None, None, "tm"),
        check_vma=False,
    )
```

```python
import functools

import jax
import jax.numpy as jnp
from jax import lax
from jax.experimental import pallas as pl
from jax.experimental.pallas import tpu as pltpu
from jax.sharding import PartitionSpec as P

TAPS = 16
MAXD = 16
RIM = 32
MESH = pl.DeviceIdType.MESH
F32 = jnp.float32
BF16 = jnp.bfloat16


RIGHT, LEFT = 0, 1


def lengths(ring):
    right = max(2, (ring - 1) * 2 // 5)
    return right, ring - 1 - right


def dot_nt(left, right):
    return lax.dot_general(left, right, (((1,), (1,)), ((), ())), preferred_element_type=F32)


def kernel(
    ring,
    blocks,
    volt,
    steer,
    sets_hbm,
    delays,
    taps_hbm,
    out,
    sets,
    taps,
    vbuf,
    wbuf,
    rim_out,
    rim_in,
    band,
    band_rim,
    top,
    own,
    send,
    recv,
    small_sem,
    load_sem,
    rim_send,
    rim_recv,
    ring_send,
    ring_recv,
):
    me = lax.axis_index("station")
    block = lax.axis_index("tm")
    per = vbuf.shape[1]
    time = vbuf.shape[3]
    rows = vbuf.shape[2]
    antennas = rows // 2
    set_count = taps.shape[0]
    sides = (lax.rem(me + 1, ring), lax.rem(me + ring - 1, ring))
    right_len, left_len = lengths(ring)

    barrier = pltpu.get_barrier_semaphore()
    for side in sides:
        pl.semaphore_signal(barrier, inc=1, device_id={"station": side}, device_id_type=MESH)

    @pl.when(block > 0)
    def _():
        pl.semaphore_signal(barrier, inc=1, device_id={"tm": block - 1}, device_id_type=MESH)

    @pl.when(block < blocks - 1)
    def _():
        pl.semaphore_signal(barrier, inc=1, device_id={"tm": block + 1}, device_id_type=MESH)

    def left_slot(step):
        return jnp.where(step < right_len, 2 * step, step + right_len)

    def right_slot(step):
        return 2 * step + 1

    def block_of(slot):
        ahead = right_len - slot // 2
        behind = left_len - slot // 2
        paired = jnp.where(slot % 2 == 1, ahead, ring - behind)
        return lax.rem(me + jnp.where(slot < 2 * right_len, paired, slot + 1), ring)

    def load(slot, which):
        source, target = ((volt, vbuf), (steer, wbuf))[which]
        at = block_of(slot) * per
        return pltpu.make_async_copy(source.at[pl.ds(at, per)], target.at[slot], load_sem.at[slot, which])

    def start_loads(slot):
        load(slot, 0).start()
        load(slot, 1).start()

    small = [
        pltpu.make_async_copy(source, target, small_sem.at[index])
        for index, (source, target) in enumerate(((taps_hbm, taps), (sets_hbm, sets)))
    ]
    for copy in small:
        copy.start()
    for slot in range(4):
        start_loads(slot)
    for copy in small:
        copy.wait()

    delay = delays[0]
    table = taps[...].astype(F32)
    lane = lax.broadcasted_iota(jnp.int32, (set_count, time), 1)
    base = jnp.zeros((set_count, time), F32)
    for tap in range(TAPS):
        base = jnp.where((lane + (tap + delay)) % time == 0, table[:, tap : tap + 1], base)
    row_at = lax.broadcasted_iota(jnp.int32, (time, time), 0)
    col_at = lax.broadcasted_iota(jnp.int32, (time, time), 1)
    for index in range(set_count):
        spread = jnp.broadcast_to(base[index : index + 1], (time, time))
        turned = pltpu.roll(spread, 0, 1, stride=1, stride_axis=0)
        band[index] = jnp.where(col_at <= row_at, turned, 0.0).astype(BF16)
        turned = pltpu.roll(spread[:RIM], RIM, 1, stride=1, stride_axis=0)
        band_rim[index] = turned[:, :RIM].astype(BF16)

    pick_row = lax.broadcasted_iota(jnp.int32, (RIM, time), 0)
    pick_col = lax.broadcasted_iota(jnp.int32, (RIM, time), 1)
    pick = jnp.where(pick_col == pick_row + (time - RIM), 1.0, 0.0).astype(BF16)

    def rim_copy(slot):
        return pltpu.make_async_remote_copy(
            src_ref=rim_out.at[slot],
            dst_ref=rim_in.at[slot],
            send_sem=rim_send.at[slot],
            recv_sem=rim_recv.at[slot],
            device_id={"tm": lax.rem(block + 1, blocks)},
            device_id_type=MESH,
        )

    def send_rim(slot):
        @pl.when(block < blocks - 1)
        def _():
            for ch in range(per):
                rim_out[slot, ch] = dot_nt(pick, vbuf[slot, ch]).astype(BF16)
            rim_copy(slot).start()

    def wait_rim(slot):
        @pl.when(block > 0)
        def _():
            rim_copy(slot).wait_recv()

    @pl.when(block == 0)
    def _():
        rim_in[...] = jnp.zeros_like(rim_in)

    def steering(slot, ch):
        real_w = wbuf[slot, ch, :antennas]
        imag_w = wbuf[slot, ch, antennas:]
        upper = jnp.concatenate([real_w, imag_w], axis=1)
        lower = jnp.concatenate([-imag_w, real_w], axis=1)
        return jnp.concatenate([upper, lower], axis=0)

    def filtered(slot, ch):
        chosen = sets[0, block_of(slot) * per + ch]
        return chosen, dot_nt(band[chosen], vbuf[slot, ch])

    def with_rim(slot, ch, chosen, early):
        return early + jnp.dot(band_rim[chosen], rim_in[slot, ch], preferred_element_type=F32)

    def beams(slot, ch):
        chosen, full = filtered(slot, ch)
        early = with_rim(slot, ch, chosen, full[:RIM])
        delayed = jnp.concatenate([early, full[RIM:]], axis=0).astype(BF16)
        return jnp.dot(delayed, steering(slot, ch), preferred_element_type=F32)

    def ring_copy(way, slot, ch, part=None):
        span = pl.ds(0, time) if part is None else part
        return pltpu.make_async_remote_copy(
            src_ref=send.at[slot, ch, span],
            dst_ref=recv.at[slot, ch, span],
            send_sem=ring_send.at[slot, ch],
            recv_sem=ring_recv.at[slot, ch],
            device_id={"station": sides[way]},
            device_id_type=MESH,
        )

    def prepare(slot):
        load(slot, 0).wait()
        send_rim(slot)

    firsts = ((LEFT, 0), (RIGHT, 1))
    for _, slot in firsts:
        load(slot, 0).wait()
    greeters = 2 + jnp.where(block > 0, 1, 0) + jnp.where(block < blocks - 1, 1, 0)
    pl.semaphore_wait(barrier, greeters)
    for _, slot in firsts:
        send_rim(slot)
    for slot in range(4, ring):
        start_loads(slot)
    for _, slot in firsts:
        load(slot, 1).wait()
    early_span, late_span = pl.ds(0, RIM), pl.ds(RIM, time - RIM)
    for ch in range(per):
        for way, slot in firsts:
            chosen, full = filtered(slot, ch)
            top[slot, ch] = full[:RIM]
            late = jnp.dot(full[RIM:].astype(BF16), steering(slot, ch), preferred_element_type=F32)
            send[slot, ch, RIM:] = late.astype(BF16)
            ring_copy(way, slot, ch, late_span).start()
    for slot in (2, 3):
        prepare(slot)
    for _, slot in firsts:
        wait_rim(slot)
    for ch in range(per):
        for way, slot in firsts:
            early = with_rim(slot, ch, sets[0, block_of(slot) * per + ch], top[slot, ch]).astype(BF16)
            early = jnp.dot(early, steering(slot, ch), preferred_element_type=F32)
            send[slot, ch, :RIM] = early.astype(BF16)
            ring_copy(way, slot, ch, early_span).start()
    for slot in (4, 5):
        prepare(slot)
    for slot in (2, 3):
        load(slot, 1).wait()
        wait_rim(slot)
    for ch in range(per):
        for slot in (2, 3):
            own[slot, ch] = beams(slot, ch)
    for slot in (6, 7):
        prepare(slot)

    lag = jnp.clip((right_len + 2 - me) // 2, 0, left_len - right_len)

    def pass_on(way, before, slot, ch):
        ring_copy(way, before, ch).wait_recv()
        total = own[slot, ch] + recv[before, ch].astype(F32)
        send[slot, ch] = total.astype(BF16)
        ring_copy(way, slot, ch).start()

    @pl.loop(1, left_len)
    def _(step):
        other = step - lag
        right_on = jnp.logical_and(other >= 1, other < right_len)
        now, later = left_slot(step), left_slot(step + 1)
        right_later = jnp.minimum(right_slot(step + 1), 2 * right_len - 1)
        right_more = step + 1 < right_len
        for ch in range(per):
            pass_on(LEFT, left_slot(step - 1), now, ch)

            @pl.when(right_on)
            def _():
                pass_on(RIGHT, right_slot(other - 1), right_slot(other), ch)

            if ch == 0:
                load(later, 1).wait()
                wait_rim(later)

                @pl.when(right_more)
                def _():
                    load(right_later, 1).wait()
                    wait_rim(right_later)

            own[later, ch] = beams(later, ch)

            @pl.when(right_more)
            def _():
                own[right_later, ch] = beams(right_later, ch)

        @pl.when(step + 3 <= left_len)
        def _():
            prepare(left_slot(step + 3))

        @pl.when(step + 3 < right_len)
        def _():
            prepare(jnp.minimum(right_slot(step + 3), 2 * right_len - 1))

    for ch in range(per):
        total = own[ring - 1, ch]
        for way, slot in ((RIGHT, 2 * right_len - 1), (LEFT, ring - 2)):
            ring_copy(way, slot, ch).wait_recv()
            total = total + recv[slot, ch].astype(F32)
        out[ch] = total.T.astype(BF16)

    @pl.loop(0, ring - 1)
    def _(slot):
        for ch in range(per):
            ring_copy(LEFT, slot, ch).wait_send()

    @pl.when(block < blocks - 1)
    def _():
        @pl.loop(0, ring)
        def _(slot):
            rim_copy(slot).wait_send()


def body(ring, blocks, voltages, delays, tap_sets, tap_table, weights):
    _, channels, parts, antennas, time = voltages.shape
    beams = weights.shape[-1]
    per = channels // ring
    rows = parts * antennas
    set_count = tap_table.shape[0]
    out = pl.pallas_call(
        functools.partial(kernel, ring, blocks),
        out_shape=jax.ShapeDtypeStruct((per, 2 * beams, time), BF16),
        in_specs=[
            pl.BlockSpec(memory_space=pltpu.HBM),
            pl.BlockSpec(memory_space=pltpu.HBM),
            pl.BlockSpec(memory_space=pltpu.HBM),
            pl.BlockSpec(memory_space=pltpu.SMEM),
            pl.BlockSpec(memory_space=pltpu.HBM),
        ],
        out_specs=pl.BlockSpec(memory_space=pltpu.VMEM),
        scratch_shapes=[
            pltpu.SMEM(tap_sets.shape, jnp.int32),
            pltpu.VMEM(tap_table.shape, BF16),
            pltpu.VMEM((ring, per, rows, time), BF16),
            pltpu.VMEM((ring, per, rows, beams), BF16),
            pltpu.VMEM((ring, per, RIM, rows), BF16),
            pltpu.VMEM((ring, per, RIM, rows), BF16),
            pltpu.VMEM((set_count, time, time), BF16),
            pltpu.VMEM((set_count, RIM, RIM), BF16),
            pltpu.VMEM((2, per, RIM, rows), F32),
            pltpu.VMEM((ring, per, time, 2 * beams), F32),
            pltpu.VMEM((ring - 1, per, time, 2 * beams), BF16),
            pltpu.VMEM((ring - 1, per, time, 2 * beams), BF16),
            pltpu.SemaphoreType.DMA((2,)),
            pltpu.SemaphoreType.DMA((ring, 2)),
            pltpu.SemaphoreType.DMA((ring,)),
            pltpu.SemaphoreType.DMA((ring,)),
            pltpu.SemaphoreType.DMA((ring - 1, per)),
            pltpu.SemaphoreType.DMA((ring - 1, per)),
        ],
        compiler_params=pltpu.CompilerParams(
            collective_id=0, has_side_effects=True, vmem_limit_bytes=63 * 1024 * 1024
        ),
    )(
        voltages.reshape(channels, rows, time),
        weights.reshape(channels, rows, beams),
        tap_sets,
        delays,
        tap_table,
    )
    return out.reshape(per, 2, beams, time)


def solution(mesh):
    return jax.shard_map(
        functools.partial(body, mesh.shape["station"], mesh.shape["tm"]),
        mesh=mesh,
        in_specs=(
            P(("group", "station"), "chan", None, None, "tm"),
            P(("group", "station")),
            P(("group", "station"), "chan"),
            P(),
            P(("group", "station"), "chan", None, None, None),
        ),
        out_specs=P(("group", "chan", "station"), None, None, "tm"),
        check_vma=False,
    )
```

```python
import functools

import jax
import jax.numpy as jnp
from jax import lax
from jax.experimental import pallas as pl
from jax.experimental.pallas import tpu as pltpu
from jax.sharding import PartitionSpec as P

TAPS = 16
MAXD = 16
RIM = 32
MESH = pl.DeviceIdType.MESH
F32 = jnp.float32
BF16 = jnp.bfloat16


def dot_nt(left, right):
    return lax.dot_general(left, right, (((1,), (1,)), ((), ())), preferred_element_type=F32)


def kernel(
    ring,
    blocks,
    volt,
    steer,
    sets_hbm,
    delays,
    taps_hbm,
    out,
    sets,
    taps,
    vbuf,
    wbuf,
    rim_out,
    rim_in,
    band,
    band_rim,
    top,
    own,
    send,
    recv,
    small_sem,
    load_sem,
    rim_send,
    rim_recv,
    ring_send,
    ring_recv,
):
    me = lax.axis_index("station")
    block = lax.axis_index("tm")
    middle = ring // 2
    per = vbuf.shape[1]
    time = vbuf.shape[3]
    rows = vbuf.shape[2]
    antennas = rows // 2
    set_count = taps.shape[0]
    sides = (lax.rem(me + 1, ring), lax.rem(me + ring - 1, ring))

    barrier = pltpu.get_barrier_semaphore()
    for side in sides:
        pl.semaphore_signal(barrier, inc=1, device_id={"station": side}, device_id_type=MESH)

    @pl.when(block > 0)
    def _():
        pl.semaphore_signal(barrier, inc=1, device_id={"tm": block - 1}, device_id_type=MESH)

    @pl.when(block < blocks - 1)
    def _():
        pl.semaphore_signal(barrier, inc=1, device_id={"tm": block + 1}, device_id_type=MESH)

    def block_of(slot):
        odd = slot % 2
        distance = jnp.where(odd == 1, ring - (slot + 1) // 2, slot // 2)
        return lax.rem(me + middle + distance, ring)

    def load(slot, which):
        source, target = ((volt, vbuf), (steer, wbuf))[which]
        at = block_of(slot) * per
        return pltpu.make_async_copy(source.at[pl.ds(at, per)], target.at[slot], load_sem.at[slot, which])

    def start_loads(slot):
        load(slot, 0).start()
        load(slot, 1).start()

    small = [
        pltpu.make_async_copy(source, target, small_sem.at[index])
        for index, (source, target) in enumerate(((taps_hbm, taps), (sets_hbm, sets)))
    ]
    for copy in small:
        copy.start()
    for slot in range(3):
        start_loads(slot)
    for copy in small:
        copy.wait()

    delay = delays[0]
    table = taps[...].astype(F32)
    lane = lax.broadcasted_iota(jnp.int32, (set_count, time), 1)
    base = jnp.zeros((set_count, time), F32)
    for tap in range(TAPS):
        base = jnp.where((lane + (tap + delay)) % time == 0, table[:, tap : tap + 1], base)
    row_at = lax.broadcasted_iota(jnp.int32, (time, time), 0)
    col_at = lax.broadcasted_iota(jnp.int32, (time, time), 1)
    for index in range(set_count):
        spread = jnp.broadcast_to(base[index : index + 1], (time, time))
        turned = pltpu.roll(spread, 0, 1, stride=1, stride_axis=0)
        band[index] = jnp.where(col_at <= row_at, turned, 0.0).astype(BF16)
        turned = pltpu.roll(spread[:RIM], RIM, 1, stride=1, stride_axis=0)
        band_rim[index] = turned[:, :RIM].astype(BF16)

    pick_row = lax.broadcasted_iota(jnp.int32, (RIM, time), 0)
    pick_col = lax.broadcasted_iota(jnp.int32, (RIM, time), 1)
    pick = jnp.where(pick_col == pick_row + (time - RIM), 1.0, 0.0).astype(BF16)

    def rim_copy(slot):
        return pltpu.make_async_remote_copy(
            src_ref=rim_out.at[slot],
            dst_ref=rim_in.at[slot],
            send_sem=rim_send.at[slot],
            recv_sem=rim_recv.at[slot],
            device_id={"tm": lax.rem(block + 1, blocks)},
            device_id_type=MESH,
        )

    def send_rim(slot):
        @pl.when(block < blocks - 1)
        def _():
            for ch in range(per):
                rim_out[slot, ch] = dot_nt(pick, vbuf[slot, ch]).astype(BF16)
            rim_copy(slot).start()

    def wait_rim(slot):
        @pl.when(block > 0)
        def _():
            rim_copy(slot).wait_recv()

    @pl.when(block == 0)
    def _():
        rim_in[...] = jnp.zeros_like(rim_in)

    def steering(slot, ch):
        real_w = wbuf[slot, ch, :antennas]
        imag_w = wbuf[slot, ch, antennas:]
        upper = jnp.concatenate([real_w, imag_w], axis=1)
        lower = jnp.concatenate([-imag_w, real_w], axis=1)
        return jnp.concatenate([upper, lower], axis=0)

    def filtered(slot, ch):
        chosen = sets[0, block_of(slot) * per + ch]
        return chosen, dot_nt(band[chosen], vbuf[slot, ch])

    def with_rim(slot, ch, chosen, early):
        return early + jnp.dot(band_rim[chosen], rim_in[slot, ch], preferred_element_type=F32)

    def beams(slot, ch):
        chosen, full = filtered(slot, ch)
        early = with_rim(slot, ch, chosen, full[:RIM])
        delayed = jnp.concatenate([early, full[RIM:]], axis=0).astype(BF16)
        return jnp.dot(delayed, steering(slot, ch), preferred_element_type=F32)

    def ring_copy(way, step, ch, part=None):
        span = pl.ds(0, time) if part is None else part
        return pltpu.make_async_remote_copy(
            src_ref=send.at[way, step, ch, span],
            dst_ref=recv.at[way, step, ch, span],
            send_sem=ring_send.at[way, step, ch],
            recv_sem=ring_recv.at[way, step, ch],
            device_id={"station": sides[way]},
            device_id_type=MESH,
        )

    half = per // 2
    order = ([(q + half) % per for q in range(per)], list(range(per)))
    first_way = [0 if ch < half else 1 for ch in range(per)]

    load(0, 0).wait()
    greeters = 2 + jnp.where(block > 0, 1, 0) + jnp.where(block < blocks - 1, 1, 0)
    pl.semaphore_wait(barrier, greeters)
    send_rim(0)
    for slot in range(3, ring):
        start_loads(slot)
    load(0, 1).wait()
    early_span, late_span = pl.ds(0, RIM), pl.ds(RIM, time - RIM)
    for q in range(half):
        for ch in (q, q + half):
            way = first_way[ch]
            chosen, full = filtered(0, ch)
            top[ch] = full[:RIM]
            late = jnp.dot(full[RIM:].astype(BF16), steering(0, ch), preferred_element_type=F32)
            send[way, 0, ch, RIM:] = late.astype(BF16)
            ring_copy(way, 0, ch, late_span).start()
    for slot in (1, 2):
        load(slot, 0).wait()
        send_rim(slot)
    wait_rim(0)
    for q in range(half):
        for ch in (q, q + half):
            way = first_way[ch]
            early = with_rim(0, ch, sets[0, block_of(0) * per + ch], top[ch]).astype(BF16)
            early = jnp.dot(early, steering(0, ch), preferred_element_type=F32)
            send[way, 0, ch, :RIM] = early.astype(BF16)
            ring_copy(way, 0, ch, early_span).start()
    for slot in (1, 2):
        load(slot, 1).wait()
        wait_rim(slot)
    for q in range(per):
        for way in (0, 1):
            own[1, way, order[way][q]] = beams(1 + way, order[way][q])
    for slot in range(3, min(7, ring)):
        load(slot, 0).wait()
        send_rim(slot)

    def one_step(step, first, last):
        now, later = step % 2, (step + 1) % 2
        coming = (2 * step + 1,) if last else (2 * step + 1, 2 * step + 2)
        for q in range(per):
            for way in (0, 1):
                ch = order[way][q]
                total = own[now, way, ch]
                if not first or q >= half:
                    ring_copy(way, step - 1, ch).wait_recv()
                    total = total + recv[way, step - 1, ch].astype(F32)
                send[way, step, ch] = total.astype(BF16)
                ring_copy(way, step, ch).start()
            if q == 0:
                for slot in coming:
                    load(slot, 1).wait()
                    wait_rim(slot)
            for way, slot in enumerate(coming):
                ch = order[way][q]
                own[later, way, ch] = beams(slot, ch)

    def prepare(slot):
        load(slot, 0).wait()
        send_rim(slot)

    for step in range(1, middle):
        if 2 <= step < middle - 2:
            continue
        if step == middle - 2 and middle - 2 > 2:

            @pl.loop(2, middle - 2)
            def _(at):
                one_step(at, False, False)
                prepare(2 * at + 5)

                @pl.when(2 * at + 6 < ring)
                def _():
                    prepare(jnp.minimum(2 * at + 6, ring - 1))

        one_step(step, step == 1, step == middle - 1)
        for slot in (2 * step + 5, 2 * step + 6):
            if slot < ring:
                prepare(slot)

    end = middle % 2
    for q in range(per):
        for way in (0, 1):
            ch = order[way][q]
            ring_copy(way, middle - 1, ch).wait_recv()
            total = own[end, 0, ch] + recv[way, middle - 1, ch].astype(F32)
            if q < half:
                own[end, 0, ch] = total
            else:
                out[ch] = total.T.astype(BF16)

    for ch in range(per):
        ring_copy(first_way[ch], 0, ch).wait_send()

    @pl.loop(1, middle)
    def _(at):
        for way in (0, 1):
            for ch in range(per):
                ring_copy(way, at, ch).wait_send()

    @pl.when(block < blocks - 1)
    def _():
        @pl.loop(0, ring)
        def _(slot):
            rim_copy(slot).wait_send()


def body(ring, blocks, voltages, delays, tap_sets, tap_table, weights):
    _, channels, parts, antennas, time = voltages.shape
    beams = weights.shape[-1]
    per = channels // ring
    rows = parts * antennas
    middle = ring // 2
    set_count = tap_table.shape[0]
    out = pl.pallas_call(
        functools.partial(kernel, ring, blocks),
        out_shape=jax.ShapeDtypeStruct((per, 2 * beams, time), BF16),
        in_specs=[
            pl.BlockSpec(memory_space=pltpu.HBM),
            pl.BlockSpec(memory_space=pltpu.HBM),
            pl.BlockSpec(memory_space=pltpu.HBM),
            pl.BlockSpec(memory_space=pltpu.SMEM),
            pl.BlockSpec(memory_space=pltpu.HBM),
        ],
        out_specs=pl.BlockSpec(memory_space=pltpu.VMEM),
        scratch_shapes=[
            pltpu.SMEM(tap_sets.shape, jnp.int32),
            pltpu.VMEM(tap_table.shape, BF16),
            pltpu.VMEM((ring, per, rows, time), BF16),
            pltpu.VMEM((ring, per, rows, beams), BF16),
            pltpu.VMEM((ring, per, RIM, rows), BF16),
            pltpu.VMEM((ring, per, RIM, rows), BF16),
            pltpu.VMEM((set_count, time, time), BF16),
            pltpu.VMEM((set_count, RIM, RIM), BF16),
            pltpu.VMEM((per, RIM, rows), F32),
            pltpu.VMEM((2, 2, per, time, 2 * beams), F32),
            pltpu.VMEM((2, middle, per, time, 2 * beams), BF16),
            pltpu.VMEM((2, middle, per, time, 2 * beams), BF16),
            pltpu.SemaphoreType.DMA((2,)),
            pltpu.SemaphoreType.DMA((ring, 2)),
            pltpu.SemaphoreType.DMA((ring,)),
            pltpu.SemaphoreType.DMA((ring,)),
            pltpu.SemaphoreType.DMA((2, middle, per)),
            pltpu.SemaphoreType.DMA((2, middle, per)),
        ],
        compiler_params=pltpu.CompilerParams(
            collective_id=0, has_side_effects=True, vmem_limit_bytes=63 * 1024 * 1024
        ),
    )(
        voltages.reshape(channels, rows, time),
        weights.reshape(channels, rows, beams),
        tap_sets,
        delays,
        tap_table,
    )
    return out.reshape(per, 2, beams, time)


def solution(mesh):
    return jax.shard_map(
        functools.partial(body, mesh.shape["station"], mesh.shape["tm"]),
        mesh=mesh,
        in_specs=(
            P(("group", "station"), "chan", None, None, "tm"),
            P(("group", "station")),
            P(("group", "station"), "chan"),
            P(),
            P(("group", "station"), "chan", None, None, None),
        ),
        out_specs=P(("group", "chan", "station"), None, None, "tm"),
        check_vma=False,
    )
```

```python
import functools

import jax
import jax.numpy as jnp
from jax import lax
from jax.experimental import pallas as pl
from jax.experimental.pallas import tpu as pltpu
from jax.sharding import PartitionSpec as P

TAPS = 16
MAXD = 16
RIM = 32
MESH = pl.DeviceIdType.MESH
F32 = jnp.float32
BF16 = jnp.bfloat16


RIGHT, LEFT = 0, 1
CUT = 2


def dot_nt(left, right):
    return lax.dot_general(left, right, (((1,), (1,)), ((), ())), preferred_element_type=F32)


def kernel(
    ring,
    blocks,
    volt,
    steer,
    sets_hbm,
    delays,
    taps_hbm,
    out,
    sets,
    taps,
    vbuf,
    wbuf,
    rim_out,
    rim_in,
    band,
    band_rim,
    top,
    own,
    send,
    recv,
    small_sem,
    load_sem,
    rim_send,
    rim_recv,
    behind_in,
    ring_send,
    ring_recv,
):
    me = lax.axis_index("station")
    block = lax.axis_index("tm")
    per = vbuf.shape[1]
    time = vbuf.shape[3]
    rows = vbuf.shape[2]
    antennas = rows // 2
    set_count = taps.shape[0]
    middle, half = ring // 2, per // 2
    sides = (lax.rem(me + 1, ring), lax.rem(me + ring - 1, ring))

    barrier = pltpu.get_barrier_semaphore()
    pl.semaphore_signal(barrier, inc=1, device_id={"station": sides[LEFT]}, device_id_type=MESH)

    @pl.when(block > 0)
    def _():
        pl.semaphore_signal(barrier, inc=1, device_id={"tm": block - 1}, device_id_type=MESH)

    def reach(way, target, ch):
        right = middle - ch // half
        inner = jnp.logical_and(target >= middle - CUT, target < middle + CUT)
        right = jnp.where(inner, target, right)
        return right if way == RIGHT else ring - 1 - right

    furthest = middle + max(CUT - 1, 0)

    def target_of(way, hops):
        return lax.rem(me + ring + (hops if way == RIGHT else -hops), ring)

    def slot_of(way, hops):
        nearer = middle - hops
        near = 2 * nearer - 1 if way == RIGHT else 2 * nearer
        far = -2 * nearer if way == RIGHT else -2 * nearer - 1
        if isinstance(hops, int):
            return near if nearer > 0 else max(far, 0)
        return jnp.where(nearer > 0, near, jnp.maximum(far, 0))

    def block_of(slot):
        odd = slot % 2
        distance = jnp.where(odd == 1, ring - (slot + 1) // 2, slot // 2)
        return lax.rem(me + middle + distance, ring)

    def load(slot, which):
        source, target = ((volt, vbuf), (steer, wbuf))[which]
        at = block_of(slot) * per
        return pltpu.make_async_copy(source.at[pl.ds(at, per)], target.at[slot], load_sem.at[slot, which])

    def start_loads(slot):
        load(slot, 0).start()
        load(slot, 1).start()

    small = [
        pltpu.make_async_copy(source, target, small_sem.at[index])
        for index, (source, target) in enumerate(((taps_hbm, taps), (sets_hbm, sets)))
    ]
    for copy in small:
        copy.start()
    for slot in range(3):
        start_loads(slot)
    for copy in small:
        copy.wait()

    delay = delays[0]
    table = taps[...].astype(F32)
    lane = lax.broadcasted_iota(jnp.int32, (set_count, time), 1)
    base = jnp.zeros((set_count, time), F32)
    for tap in range(TAPS):
        base = jnp.where((lane + (tap + delay)) % time == 0, table[:, tap : tap + 1], base)
    row_at = lax.broadcasted_iota(jnp.int32, (time, time), 0)
    col_at = lax.broadcasted_iota(jnp.int32, (time, time), 1)
    for index in range(set_count):
        spread = jnp.broadcast_to(base[index : index + 1], (time, time))
        turned = pltpu.roll(spread, 0, 1, stride=1, stride_axis=0)
        band[index] = jnp.where(col_at <= row_at, turned, 0.0).astype(BF16)
        turned = pltpu.roll(spread[:RIM], RIM, 1, stride=1, stride_axis=0)
        band_rim[index] = turned[:, :RIM].astype(BF16)

    pick_row = lax.broadcasted_iota(jnp.int32, (RIM, time), 0)
    pick_col = lax.broadcasted_iota(jnp.int32, (RIM, time), 1)
    pick = jnp.where(pick_col == pick_row + (time - RIM), 1.0, 0.0).astype(BF16)

    def rim_copy(slot, part):
        pair = pl.ds(part * half, half)
        return pltpu.make_async_remote_copy(
            src_ref=rim_out.at[slot, pair],
            dst_ref=rim_in.at[slot, pair],
            send_sem=rim_send.at[slot, part],
            recv_sem=rim_recv.at[slot, part],
            device_id={"tm": lax.rem(block + 1, blocks)},
            device_id_type=MESH,
        )

    def send_rim(slot, part):
        @pl.when(block < blocks - 1)
        def _():
            for ch in range(part * half, (part + 1) * half):
                rim_out[slot, ch] = dot_nt(pick, vbuf[slot, ch]).astype(BF16)
            rim_copy(slot, part).start()

    def wait_rim(slot, part):
        @pl.when(block > 0)
        def _():
            rim_copy(slot, part).wait_recv()

    @pl.when(block == 0)
    def _():
        rim_in[...] = jnp.zeros_like(rim_in)

    def steering(slot, ch):
        real_w = wbuf[slot, ch, :antennas]
        imag_w = wbuf[slot, ch, antennas:]
        upper = jnp.concatenate([real_w, imag_w], axis=1)
        lower = jnp.concatenate([-imag_w, real_w], axis=1)
        return jnp.concatenate([upper, lower], axis=0)

    def filtered(slot, ch):
        chosen = sets[0, block_of(slot) * per + ch]
        return chosen, dot_nt(band[chosen], vbuf[slot, ch])

    def with_rim(slot, ch, chosen, early):
        return early + jnp.dot(band_rim[chosen], rim_in[slot, ch], preferred_element_type=F32)

    def beams(slot, ch):
        chosen, full = filtered(slot, ch)
        early = with_rim(slot, ch, chosen, full[:RIM])
        delayed = jnp.concatenate([early, full[RIM:]], axis=0).astype(BF16)
        return jnp.dot(delayed, steering(slot, ch), preferred_element_type=F32)

    def ring_copy(way, hops, ch, part=None):
        span = pl.ds(0, time) if part is None else part
        return pltpu.make_async_remote_copy(
            src_ref=send.at[way, hops, ch, span],
            dst_ref=recv.at[way, hops, ch, span],
            send_sem=ring_send.at[way, hops, ch],
            recv_sem=ring_recv.at[way, hops, ch],
            device_id={"station": sides[way]},
            device_id_type=MESH,
        )

    def starts(way, hops, ch):
        return reach(way, target_of(way, hops), ch) == hops

    firsts = []
    for back in (0, 1):
        for q in range(half):
            firsts.append((RIGHT, middle - back, back * half + q))
            firsts.append((LEFT, middle - back, (1 - back) * half + q))
    early_span, late_span = pl.ds(0, RIM), pl.ds(RIM, time - RIM)

    def enter_left():
        pl.semaphore_wait(behind_in, 1)

    def late_part(index):
        way, hops, ch = firsts[index]
        slot = slot_of(way, hops)
        chosen, full = filtered(slot, ch)
        top[index] = full[:RIM]
        late = jnp.dot(full[RIM:].astype(BF16), steering(slot, ch), preferred_element_type=F32)
        send[way, hops, ch, RIM:] = late.astype(BF16)

    def early_part(index):
        way, hops, ch = firsts[index]
        slot = slot_of(way, hops)
        chosen = sets[0, block_of(slot) * per + ch]
        early = with_rim(slot, ch, chosen, top[index]).astype(BF16)
        early = jnp.dot(early, steering(slot, ch), preferred_element_type=F32)
        send[way, hops, ch, :RIM] = early.astype(BF16)

    def leave(index, span):
        way, hops, ch = firsts[index]

        @pl.when(starts(way, hops, ch))
        def _():
            ring_copy(way, hops, ch, span).start()

    load(0, 0).wait()
    load(0, 1).wait()
    for index in range(2 * half):
        late_part(index)
    pl.semaphore_wait(barrier, 1 + jnp.where(block < blocks - 1, 1, 0))
    pl.semaphore_signal(behind_in, inc=1, device_id={"station": sides[RIGHT]}, device_id_type=MESH)

    if CUT:

        @pl.when(me > 0)
        def _():
            enter_left()
    else:
        enter_left()

    for index in range(2 * half):
        leave(index, late_span)
    for part in (0, 1):
        send_rim(0, part)
    for slot in (1, 2):
        load(slot, 0).wait()
        send_rim(slot, 2 - slot)
    for slot in (1, 2):
        load(slot, 1).wait()
    for index in range(2 * half, 4 * half):
        late_part(index)
        leave(index, late_span)
    for slot in range(3, ring):
        start_loads(slot)
    for slot in (1, 2):
        send_rim(slot, slot - 1)
    for part in (0, 1):
        wait_rim(0, part)
    for index in range(2 * half):
        early_part(index)
        leave(index, early_span)
    for slot in (1, 2):
        wait_rim(slot, 2 - slot)
    for index in range(2 * half, 4 * half):
        early_part(index)
        leave(index, early_span)

    def prepare(slot):
        load(slot, 0).wait()
        for part in (0, 1):
            send_rim(slot, part)

    def fill(slots):
        for slot in slots:
            load(slot, 1).wait()
            for part in (0, 1):
                wait_rim(slot, part)

    prepare(3)
    prepare(4)
    for slot in (1, 2):
        wait_rim(slot, slot - 1)
    for ch in range(per):
        for slot in (0, 1, 2):
            own[slot, ch] = beams(slot, ch)
    prepare(5)
    prepare(6)

    lags = [0, 0]
    if CUT:
        lags[RIGHT] = jnp.where(jnp.logical_and(me >= 1, me <= CUT), 1, 0)
        lags[LEFT] = jnp.clip((middle - (ring - 1 - me)) // 2, 0, 3)
    order = ([(q + half) % per for q in range(per)], list(range(per)))

    def pass_on(way, hops, ch):
        slot = slot_of(way, hops)
        length = reach(way, target_of(way, hops), ch)
        begun = hops == (middle if (ch < half) == (way == RIGHT) else middle - 1)
        within = jnp.logical_and(hops >= 1, hops <= furthest)

        if CUT:

            @pl.when(jnp.logical_and(within, jnp.logical_and(length == hops, jnp.logical_not(begun))))
            def _():
                send[way, hops, ch] = own[slot, ch].astype(BF16)
                ring_copy(way, hops, ch).start()

        @pl.when(jnp.logical_and(within, length > hops))
        def _():
            ring_copy(way, hops + 1, ch).wait_recv()
            total = own[slot, ch] + recv[way, hops + 1, ch].astype(F32)
            send[way, hops, ch] = total.astype(BF16)
            ring_copy(way, hops, ch).start()

    count = furthest + (3 if CUT else 0)

    @pl.loop(0, count)
    def _(step):
        hops = [furthest - step + lags[way] for way in (RIGHT, LEFT)]
        coming = middle - 2 - step
        slots = [slot_of(way, jnp.maximum(coming, 1)) for way in (RIGHT, LEFT)]

        if CUT:
            @pl.when(jnp.logical_and(me == 0, step == CUT + 1))
            def _():
                enter_left()

        for q in range(per):
            pass_on(LEFT, hops[LEFT], order[LEFT][q])
            pass_on(RIGHT, hops[RIGHT], order[RIGHT][q])

            @pl.when(coming >= 1)
            def _():
                if q == 0:
                    fill(slots)
                for way in (RIGHT, LEFT):
                    ch = order[way][q]
                    own[slots[way], ch] = beams(slots[way], ch)

            @pl.when(coming == 0)
            def _():
                if q == 0:
                    fill((ring - 1,))
                own[ring - 1, q] = beams(ring - 1, q)

        @pl.when(coming >= 3)
        def _():
            for way in (RIGHT, LEFT):
                prepare(slot_of(way, jnp.maximum(coming - 2, 1)))

        @pl.when(coming == 2)
        def _():
            prepare(ring - 1)

    for q in range(per):
        for way in (RIGHT, LEFT):
            ch = order[way][q]
            ring_copy(way, 1, ch).wait_recv()
            total = own[ring - 1, ch] + recv[way, 1, ch].astype(F32)
            if q < half:
                own[ring - 1, ch] = total
            else:
                out[ch] = total.T.astype(BF16)

    @pl.loop(1, furthest + 1)
    def _(hops):
        for way in (RIGHT, LEFT):
            for ch in range(per):

                @pl.when(reach(way, target_of(way, hops), ch) >= hops)
                def _():
                    ring_copy(way, hops, ch).wait_send()

    @pl.when(block < blocks - 1)
    def _():
        @pl.loop(0, ring)
        def _(slot):
            for part in (0, 1):
                rim_copy(slot, part).wait_send()


def body(ring, blocks, voltages, delays, tap_sets, tap_table, weights):
    _, channels, parts, antennas, time = voltages.shape
    beams = weights.shape[-1]
    per = channels // ring
    rows = parts * antennas
    hops = ring // 2 + max(CUT - 1, 0) + 1
    set_count = tap_table.shape[0]
    out = pl.pallas_call(
        functools.partial(kernel, ring, blocks),
        out_shape=jax.ShapeDtypeStruct((per, 2 * beams, time), BF16),
        in_specs=[
            pl.BlockSpec(memory_space=pltpu.HBM),
            pl.BlockSpec(memory_space=pltpu.HBM),
            pl.BlockSpec(memory_space=pltpu.HBM),
            pl.BlockSpec(memory_space=pltpu.SMEM),
            pl.BlockSpec(memory_space=pltpu.HBM),
        ],
        out_specs=pl.BlockSpec(memory_space=pltpu.VMEM),
        scratch_shapes=[
            pltpu.SMEM(tap_sets.shape, jnp.int32),
            pltpu.VMEM(tap_table.shape, BF16),
            pltpu.VMEM((ring, per, rows, time), BF16),
            pltpu.VMEM((ring, per, rows, beams), BF16),
            pltpu.VMEM((ring, per, RIM, rows), BF16),
            pltpu.VMEM((ring, per, RIM, rows), BF16),
            pltpu.VMEM((set_count, time, time), BF16),
            pltpu.VMEM((set_count, RIM, RIM), BF16),
            pltpu.VMEM((2 * per, RIM, rows), F32),
            pltpu.VMEM((ring, per, time, 2 * beams), F32),
            pltpu.VMEM((2, hops, per, time, 2 * beams), BF16),
            pltpu.VMEM((2, hops, per, time, 2 * beams), BF16),
            pltpu.SemaphoreType.DMA((2,)),
            pltpu.SemaphoreType.DMA((ring, 2)),
            pltpu.SemaphoreType.DMA((ring, 2)),
            pltpu.SemaphoreType.DMA((ring, 2)),
            pltpu.SemaphoreType.REGULAR,
            pltpu.SemaphoreType.DMA((2, hops, per)),
            pltpu.SemaphoreType.DMA((2, hops, per)),
        ],
        compiler_params=pltpu.CompilerParams(
            collective_id=0, has_side_effects=True, vmem_limit_bytes=63 * 1024 * 1024
        ),
    )(
        voltages.reshape(channels, rows, time),
        weights.reshape(channels, rows, beams),
        tap_sets,
        delays,
        tap_table,
    )
    return out.reshape(per, 2, beams, time)


def solution(mesh):
    return jax.shard_map(
        functools.partial(body, mesh.shape["station"], mesh.shape["tm"]),
        mesh=mesh,
        in_specs=(
            P(("group", "station"), "chan", None, None, "tm"),
            P(("group", "station")),
            P(("group", "station"), "chan"),
            P(),
            P(("group", "station"), "chan", None, None, None),
        ),
        out_specs=P(("group", "chan", "station"), None, None, "tm"),
        check_vma=False,
    )
```

```python
import functools

import jax
import jax.numpy as jnp
from jax import lax
from jax.experimental import pallas as pl
from jax.experimental.pallas import tpu as pltpu
from jax.sharding import PartitionSpec as P

TAPS = 16
MAXD = 16
RIM = 32
MESH = pl.DeviceIdType.MESH
F32 = jnp.float32
BF16 = jnp.bfloat16


RIGHT, LEFT = 0, 1


def dot_nt(left, right):
    return lax.dot_general(left, right, (((1,), (1,)), ((), ())), preferred_element_type=F32)


def kernel(
    ring,
    blocks,
    volt,
    steer,
    sets_hbm,
    delays,
    taps_hbm,
    out,
    sets,
    taps,
    vbuf,
    wbuf,
    rim_out,
    rim_in,
    band,
    band_rim,
    top,
    own,
    send,
    recv,
    small_sem,
    load_sem,
    rim_send,
    rim_recv,
    ring_send,
    ring_recv,
):
    me = lax.axis_index("station")
    block = lax.axis_index("tm")
    per = vbuf.shape[1]
    time = vbuf.shape[3]
    rows = vbuf.shape[2]
    antennas = rows // 2
    set_count = taps.shape[0]
    middle, half = ring // 2, per // 2
    sides = (lax.rem(me + 1, ring), lax.rem(me + ring - 1, ring))

    barrier = pltpu.get_barrier_semaphore()
    for side in sides:
        pl.semaphore_signal(barrier, inc=1, device_id={"station": side}, device_id_type=MESH)

    @pl.when(block > 0)
    def _():
        pl.semaphore_signal(barrier, inc=1, device_id={"tm": block - 1}, device_id_type=MESH)

    @pl.when(block < blocks - 1)
    def _():
        pl.semaphore_signal(barrier, inc=1, device_id={"tm": block + 1}, device_id_type=MESH)

    def reach(way, ch):
        right = middle - ch // half
        return right if way == RIGHT else ring - 1 - right

    def slot_of(way, hops):
        nearer = middle - hops
        near = 2 * nearer - 1 if way == RIGHT else 2 * nearer
        return max(near, 0) if isinstance(hops, int) else jnp.maximum(near, 0)

    def block_of(slot):
        odd = slot % 2
        distance = jnp.where(odd == 1, ring - (slot + 1) // 2, slot // 2)
        return lax.rem(me + middle + distance, ring)

    def load(slot, which):
        source, target = ((volt, vbuf), (steer, wbuf))[which]
        at = block_of(slot) * per
        return pltpu.make_async_copy(source.at[pl.ds(at, per)], target.at[slot], load_sem.at[slot, which])

    def start_loads(slot):
        load(slot, 0).start()
        load(slot, 1).start()

    small = [
        pltpu.make_async_copy(source, target, small_sem.at[index])
        for index, (source, target) in enumerate(((taps_hbm, taps), (sets_hbm, sets)))
    ]
    for copy in small:
        copy.start()
    for slot in range(3):
        start_loads(slot)
    for copy in small:
        copy.wait()

    delay = delays[0]
    table = taps[...].astype(F32)
    lane = lax.broadcasted_iota(jnp.int32, (set_count, time), 1)
    base = jnp.zeros((set_count, time), F32)
    for tap in range(TAPS):
        base = jnp.where((lane + (tap + delay)) % time == 0, table[:, tap : tap + 1], base)
    row_at = lax.broadcasted_iota(jnp.int32, (time, time), 0)
    col_at = lax.broadcasted_iota(jnp.int32, (time, time), 1)
    for index in range(set_count):
        spread = jnp.broadcast_to(base[index : index + 1], (time, time))
        turned = pltpu.roll(spread, 0, 1, stride=1, stride_axis=0)
        band[index] = jnp.where(col_at <= row_at, turned, 0.0).astype(BF16)
        turned = pltpu.roll(spread[:RIM], RIM, 1, stride=1, stride_axis=0)
        band_rim[index] = turned[:, :RIM].astype(BF16)

    pick_row = lax.broadcasted_iota(jnp.int32, (RIM, time), 0)
    pick_col = lax.broadcasted_iota(jnp.int32, (RIM, time), 1)
    pick = jnp.where(pick_col == pick_row + (time - RIM), 1.0, 0.0).astype(BF16)

    def rim_copy(slot, part):
        pair = pl.ds(part * half, half)
        return pltpu.make_async_remote_copy(
            src_ref=rim_out.at[slot, pair],
            dst_ref=rim_in.at[slot, pair],
            send_sem=rim_send.at[slot, part],
            recv_sem=rim_recv.at[slot, part],
            device_id={"tm": lax.rem(block + 1, blocks)},
            device_id_type=MESH,
        )

    def send_rim(slot, part):
        @pl.when(block < blocks - 1)
        def _():
            for ch in range(part * half, (part + 1) * half):
                rim_out[slot, ch] = dot_nt(pick, vbuf[slot, ch]).astype(BF16)
            rim_copy(slot, part).start()

    def wait_rim(slot, part):
        @pl.when(block > 0)
        def _():
            rim_copy(slot, part).wait_recv()

    @pl.when(block == 0)
    def _():
        rim_in[...] = jnp.zeros_like(rim_in)

    def steering(slot, ch):
        real_w = wbuf[slot, ch, :antennas]
        imag_w = wbuf[slot, ch, antennas:]
        upper = jnp.concatenate([real_w, imag_w], axis=1)
        lower = jnp.concatenate([-imag_w, real_w], axis=1)
        return jnp.concatenate([upper, lower], axis=0)

    def filtered(slot, ch):
        chosen = sets[0, block_of(slot) * per + ch]
        return chosen, dot_nt(band[chosen], vbuf[slot, ch])

    def with_rim(slot, ch, chosen, early):
        return early + jnp.dot(band_rim[chosen], rim_in[slot, ch], preferred_element_type=F32)

    def beams(slot, ch):
        chosen, full = filtered(slot, ch)
        early = with_rim(slot, ch, chosen, full[:RIM])
        delayed = jnp.concatenate([early, full[RIM:]], axis=0).astype(BF16)
        return jnp.dot(delayed, steering(slot, ch), preferred_element_type=F32)

    def ring_copy(way, hops, ch, part=None):
        span = pl.ds(0, time) if part is None else part
        return pltpu.make_async_remote_copy(
            src_ref=send.at[way, hops, ch, span],
            dst_ref=recv.at[way, hops, ch, span],
            send_sem=ring_send.at[way, hops, ch],
            recv_sem=ring_recv.at[way, hops, ch],
            device_id={"station": sides[way]},
            device_id_type=MESH,
        )

    firsts = []
    for back in (0, 1):
        for q in range(half):
            firsts.append((RIGHT, middle - back, back * half + q))
            firsts.append((LEFT, middle - back, (1 - back) * half + q))
    early_span, late_span = pl.ds(0, RIM), pl.ds(RIM, time - RIM)

    def late_part(index):
        way, hops, ch = firsts[index]
        slot = slot_of(way, hops)
        chosen, full = filtered(slot, ch)
        top[index] = full[:RIM]
        late = jnp.dot(full[RIM:].astype(BF16), steering(slot, ch), preferred_element_type=F32)
        send[way, hops, ch, RIM:] = late.astype(BF16)

    def early_part(index):
        way, hops, ch = firsts[index]
        slot = slot_of(way, hops)
        chosen = sets[0, block_of(slot) * per + ch]
        early = with_rim(slot, ch, chosen, top[index]).astype(BF16)
        early = jnp.dot(early, steering(slot, ch), preferred_element_type=F32)
        send[way, hops, ch, :RIM] = early.astype(BF16)

    def leave(index, span):
        way, hops, ch = firsts[index]
        ring_copy(way, hops, ch, span).start()

    load(0, 0).wait()
    load(0, 1).wait()
    for index in range(2 * half):
        late_part(index)
    greeters = 2 + jnp.where(block > 0, 1, 0) + jnp.where(block < blocks - 1, 1, 0)
    pl.semaphore_wait(barrier, greeters)
    for index in range(2 * half):
        leave(index, late_span)
    for part in (0, 1):
        send_rim(0, part)
    for slot in (1, 2):
        load(slot, 0).wait()
        send_rim(slot, 2 - slot)
    for slot in (1, 2):
        load(slot, 1).wait()
    for index in range(2 * half, 4 * half):
        late_part(index)
        leave(index, late_span)
    for slot in range(3, ring):
        start_loads(slot)
    for slot in (1, 2):
        send_rim(slot, slot - 1)
    for part in (0, 1):
        wait_rim(0, part)
    for index in range(2 * half):
        early_part(index)
        leave(index, early_span)
    for slot in (1, 2):
        wait_rim(slot, 2 - slot)
    for index in range(2 * half, 4 * half):
        early_part(index)
        leave(index, early_span)

    def prepare(slot):
        load(slot, 0).wait()
        for part in (0, 1):
            send_rim(slot, part)

    def fill(slots):
        for slot in slots:
            load(slot, 1).wait()
            for part in (0, 1):
                wait_rim(slot, part)

    prepare(3)
    prepare(4)
    for slot in (1, 2):
        wait_rim(slot, slot - 1)
    for ch in range(half):
        own[1, ch] = beams(1, ch)
        own[2, ch + half] = beams(2, ch + half)
    prepare(5)
    prepare(6)

    order = ([(q + half) % per for q in range(per)], list(range(per)))

    def pass_on(way, hops, ch):
        slot = slot_of(way, hops)

        @pl.when(reach(way, ch) > hops)
        def _():
            ring_copy(way, hops + 1, ch).wait_recv()
            total = own[slot, ch] + recv[way, hops + 1, ch].astype(F32)
            send[way, hops, ch] = total.astype(BF16)
            ring_copy(way, hops, ch).start()

    @pl.loop(1, middle)
    def _(step):
        hops = middle - step
        coming = hops - 1
        slots = [slot_of(way, jnp.maximum(coming, 1)) for way in (RIGHT, LEFT)]

        for q in range(per):
            pass_on(LEFT, hops, order[LEFT][q])
            pass_on(RIGHT, hops, order[RIGHT][q])

            @pl.when(coming >= 1)
            def _():
                if q == 0:
                    fill(slots)
                for way in (RIGHT, LEFT):
                    ch = order[way][q]
                    own[slots[way], ch] = beams(slots[way], ch)

            @pl.when(coming == 0)
            def _():
                if q == 0:
                    fill((ring - 1,))
                own[ring - 1, q] = beams(ring - 1, q)

        @pl.when(coming >= 3)
        def _():
            for way in (RIGHT, LEFT):
                prepare(slot_of(way, jnp.maximum(coming - 2, 1)))

        @pl.when(coming == 2)
        def _():
            prepare(ring - 1)

    for q in range(per):
        for way in (RIGHT, LEFT):
            ch = order[way][q]
            ring_copy(way, 1, ch).wait_recv()
            total = own[ring - 1, ch] + recv[way, 1, ch].astype(F32)
            if q < half:
                own[ring - 1, ch] = total
            else:
                out[ch] = total.T.astype(BF16)

    @pl.loop(1, middle + 1)
    def _(hops):
        for way in (RIGHT, LEFT):
            for ch in range(per):

                @pl.when(reach(way, ch) >= hops)
                def _():
                    ring_copy(way, hops, ch).wait_send()

    @pl.when(block < blocks - 1)
    def _():
        @pl.loop(0, ring)
        def _(slot):
            for part in (0, 1):
                rim_copy(slot, part).wait_send()


def body(ring, blocks, voltages, delays, tap_sets, tap_table, weights):
    _, channels, parts, antennas, time = voltages.shape
    beams = weights.shape[-1]
    per = channels // ring
    rows = parts * antennas
    hops = ring // 2 + 1
    set_count = tap_table.shape[0]
    out = pl.pallas_call(
        functools.partial(kernel, ring, blocks),
        out_shape=jax.ShapeDtypeStruct((per, 2 * beams, time), BF16),
        in_specs=[
            pl.BlockSpec(memory_space=pltpu.HBM),
            pl.BlockSpec(memory_space=pltpu.HBM),
            pl.BlockSpec(memory_space=pltpu.HBM),
            pl.BlockSpec(memory_space=pltpu.SMEM),
            pl.BlockSpec(memory_space=pltpu.HBM),
        ],
        out_specs=pl.BlockSpec(memory_space=pltpu.VMEM),
        scratch_shapes=[
            pltpu.SMEM(tap_sets.shape, jnp.int32),
            pltpu.VMEM(tap_table.shape, BF16),
            pltpu.VMEM((ring, per, rows, time), BF16),
            pltpu.VMEM((ring, per, rows, beams), BF16),
            pltpu.VMEM((ring, per, RIM, rows), BF16),
            pltpu.VMEM((ring, per, RIM, rows), BF16),
            pltpu.VMEM((set_count, time, time), BF16),
            pltpu.VMEM((set_count, RIM, RIM), BF16),
            pltpu.VMEM((2 * per, RIM, rows), F32),
            pltpu.VMEM((ring, per, time, 2 * beams), F32),
            pltpu.VMEM((2, hops, per, time, 2 * beams), BF16),
            pltpu.VMEM((2, hops, per, time, 2 * beams), BF16),
            pltpu.SemaphoreType.DMA((2,)),
            pltpu.SemaphoreType.DMA((ring, 2)),
            pltpu.SemaphoreType.DMA((ring, 2)),
            pltpu.SemaphoreType.DMA((ring, 2)),
            pltpu.SemaphoreType.DMA((2, hops, per)),
            pltpu.SemaphoreType.DMA((2, hops, per)),
        ],
        compiler_params=pltpu.CompilerParams(
            collective_id=0, has_side_effects=True, vmem_limit_bytes=63 * 1024 * 1024
        ),
    )(
        voltages.reshape(channels, rows, time),
        weights.reshape(channels, rows, beams),
        tap_sets,
        delays,
        tap_table,
    )
    return out.reshape(per, 2, beams, time)


def solution(mesh):
    return jax.shard_map(
        functools.partial(body, mesh.shape["station"], mesh.shape["tm"]),
        mesh=mesh,
        in_specs=(
            P(("group", "station"), "chan", None, None, "tm"),
            P(("group", "station")),
            P(("group", "station"), "chan"),
            P(),
            P(("group", "station"), "chan", None, None, None),
        ),
        out_specs=P(("group", "chan", "station"), None, None, "tm"),
        check_vma=False,
    )
```

```python
import functools

import jax
import jax.numpy as jnp
from jax import lax
from jax.experimental import pallas as pl
from jax.experimental.pallas import tpu as pltpu
from jax.sharding import PartitionSpec as P

TAPS = 16
MAXD = 16
RIM = 32
MESH = pl.DeviceIdType.MESH
F32 = jnp.float32
BF16 = jnp.bfloat16


OURS, THEIRS = 0, 1
CUT = 2


def dot_nt(left, right):
    return lax.dot_general(left, right, (((1,), (1,)), ((), ())), preferred_element_type=F32)


def kernel(
    ring,
    blocks,
    volt,
    steer,
    sets_hbm,
    delays,
    taps_hbm,
    out,
    sets,
    taps,
    vbuf,
    wbuf,
    rim_out,
    rim_in,
    band,
    band_rim,
    top,
    own,
    give,
    lent,
    send,
    start,
    recv,
    last,
    small_sem,
    load_sem,
    rim_send,
    rim_recv,
    ring_send,
    start_send,
    ring_recv,
    last_recv,
    give_send,
    give_recv,
    wrap_in,
):
    me = lax.axis_index("station")
    block = lax.axis_index("tm")
    core = lax.axis_index("chan")
    partner = 1 - core
    per = vbuf.shape[1]
    time = vbuf.shape[3]
    rows = vbuf.shape[2]
    antennas = rows // 2
    set_count = taps.shape[0]
    middle, half = ring // 2, per // 2
    furthest = middle + CUT - 1

    sign = 1 - 2 * core
    ahead = lax.rem(me + ring + sign, ring)
    behind = lax.rem(me + ring - sign, ring)
    right, left = lax.rem(me + 1, ring), lax.rem(me + ring - 1, ring)

    barrier = pltpu.get_barrier_semaphore()
    first_left = jnp.logical_and(me == 0, core == 1)
    last_left = jnp.logical_and(me == ring - 1, core == 1)
    at_wrap = jnp.logical_or(last_left, jnp.logical_and(me == 0, core == 0))

    def greet(**where):
        pl.semaphore_signal(barrier, inc=1, device_id=where, device_id_type=MESH)

    greet(station=left, chan=0)
    greet(chan=partner)

    @pl.when(me < ring - 1)
    def _():
        greet(station=right, chan=1)

    @pl.when(jnp.logical_not(at_wrap))
    def _():
        greet(station=behind, chan=partner)

    @pl.when(first_left)
    def _():
        greet(station=left, chan=1)

    @pl.when(block > 0)
    def _():
        greet(tm=block - 1)

    def one(flag):
        return jnp.where(flag, 1, 0)

    greeters = (
        3 - 2 * one(first_left) + one(jnp.logical_not(at_wrap)) + one(last_left) + one(block < blocks - 1)
    )

    def reach(way, target, q):
        inner = jnp.logical_and(target >= middle - CUT, target < middle + CUT)
        turned = jnp.where(core == way, target, ring - 1 - target)
        return jnp.where(inner, turned, middle - q // half)

    def target_of(way, hops):
        return lax.rem(me + ring + (sign if way == OURS else -sign) * hops, ring)

    def length(way, hops, q):
        return reach(way, target_of(way, hops), q)

    def channel(way, q):
        return lax.rem(q + (core if way == OURS else partner) * half, per)

    def is_first(hops, q):
        return hops == (middle if q < half else middle - 1)

    def slot_of(way, hops):
        nearer = middle - hops
        near = 2 * nearer - 1 if way == OURS else 2 * nearer
        far = -2 * nearer if way == OURS else -2 * nearer - 1
        if isinstance(hops, int):
            return near if nearer > 0 else max(far, 0)
        return jnp.where(nearer > 0, near, jnp.maximum(far, 0))

    def block_of(slot):
        nearer = middle - (slot + 1) // 2
        distance = jnp.where(slot % 2 == 1, sign, -sign) * nearer
        return lax.rem(me + ring + distance, ring)

    def load(slot, which):
        source, target = ((volt, vbuf), (steer, wbuf))[which]
        at = block_of(slot) * per
        return pltpu.make_async_copy(source.at[pl.ds(at, per)], target.at[slot], load_sem.at[slot, which])

    def start_loads(slot):
        load(slot, 0).start()
        load(slot, 1).start()

    small = [
        pltpu.make_async_copy(source, target, small_sem.at[index])
        for index, (source, target) in enumerate(((taps_hbm, taps), (sets_hbm, sets)))
    ]
    for copy in small:
        copy.start()
    for slot in range(3):
        start_loads(slot)
    for copy in small:
        copy.wait()

    delay = delays[0]
    table = taps[...].astype(F32)
    lane = lax.broadcasted_iota(jnp.int32, (set_count, time), 1)
    base = jnp.zeros((set_count, time), F32)
    for tap in range(TAPS):
        base = jnp.where((lane + (tap + delay)) % time == 0, table[:, tap : tap + 1], base)
    row_at = lax.broadcasted_iota(jnp.int32, (time, time), 0)
    col_at = lax.broadcasted_iota(jnp.int32, (time, time), 1)
    for index in range(set_count):
        spread = jnp.broadcast_to(base[index : index + 1], (time, time))
        turned = pltpu.roll(spread, 0, 1, stride=1, stride_axis=0)
        band[index] = jnp.where(col_at <= row_at, turned, 0.0).astype(BF16)
        turned = pltpu.roll(spread[:RIM], RIM, 1, stride=1, stride_axis=0)
        band_rim[index] = turned[:, :RIM].astype(BF16)

    pick_row = lax.broadcasted_iota(jnp.int32, (RIM, time), 0)
    pick_col = lax.broadcasted_iota(jnp.int32, (RIM, time), 1)
    pick = jnp.where(pick_col == pick_row + (time - RIM), 1.0, 0.0).astype(BF16)

    def rim_copy(slot, part):
        pair = pl.ds(part * half, half)
        return pltpu.make_async_remote_copy(
            src_ref=rim_out.at[slot, pair],
            dst_ref=rim_in.at[slot, pair],
            send_sem=rim_send.at[slot, part],
            recv_sem=rim_recv.at[slot, part],
            device_id={"tm": lax.rem(block + 1, blocks)},
            device_id_type=MESH,
        )

    def send_rim(slot, part):
        @pl.when(block < blocks - 1)
        def _():
            for q in range(half):
                ch = part * half + q
                rim_out[slot, ch] = dot_nt(pick, vbuf[slot, ch]).astype(BF16)
            rim_copy(slot, part).start()

    def wait_rim(slot, part):
        @pl.when(block > 0)
        def _():
            rim_copy(slot, part).wait_recv()

    @pl.when(block == 0)
    def _():
        rim_in[...] = jnp.zeros_like(rim_in)

    def steering(slot, ch):
        real_w = wbuf[slot, ch, :antennas]
        imag_w = wbuf[slot, ch, antennas:]
        upper = jnp.concatenate([real_w, imag_w], axis=1)
        lower = jnp.concatenate([-imag_w, real_w], axis=1)
        return jnp.concatenate([upper, lower], axis=0)

    def filtered(slot, ch):
        chosen = sets[0, block_of(slot) * per + ch]
        return chosen, dot_nt(band[chosen], vbuf[slot, ch])

    def with_rim(slot, ch, chosen, early):
        return early + jnp.dot(band_rim[chosen], rim_in[slot, ch], preferred_element_type=F32)

    def beams(slot, ch):
        chosen, full = filtered(slot, ch)
        early = with_rim(slot, ch, chosen, full[:RIM])
        delayed = jnp.concatenate([early, full[RIM:]], axis=0).astype(BF16)
        return jnp.dot(delayed, steering(slot, ch), preferred_element_type=F32)

    def pass_copy(hops, rel, q, part=None):
        span = pl.ds(0, time) if part is None else part
        return pltpu.make_async_remote_copy(
            src_ref=send.at[hops, rel, q, span],
            dst_ref=recv.at[hops, rel, q, span],
            send_sem=ring_send.at[hops, rel, q],
            recv_sem=ring_recv.at[hops, rel, q],
            device_id={"station": ahead, "chan": core},
            device_id_type=MESH,
        )

    def last_copy(way, rel, q):
        return pltpu.make_async_remote_copy(
            src_ref=send.at[1, rel, q],
            dst_ref=last.at[way, q],
            send_sem=ring_send.at[1, rel, q],
            recv_sem=last_recv.at[way, q],
            device_id={"station": ahead, "chan": partner if rel else core},
            device_id_type=MESH,
        )

    def start_copy(hops, q, part=None):
        span = pl.ds(0, time) if part is None else part
        return pltpu.make_async_remote_copy(
            src_ref=start.at[hops, q, span],
            dst_ref=recv.at[hops, 1, q, span],
            send_sem=start_send.at[hops, q],
            recv_sem=ring_recv.at[hops, 1, q],
            device_id={"station": behind, "chan": partner},
            device_id_type=MESH,
        )

    def give_copy(hops, q):
        return pltpu.make_async_remote_copy(
            src_ref=give.at[hops, q],
            dst_ref=lent.at[hops, q],
            send_sem=give_send.at[hops, q],
            recv_sem=give_recv.at[hops, q],
            device_id={"chan": partner},
            device_id_type=MESH,
        )

    firsts = []
    for back in (0, 1):
        for q in range(half):
            for way in (OURS, THEIRS):
                firsts.append((way, middle - back, back * half + q))
    early_span, late_span = pl.ds(0, RIM), pl.ds(RIM, time - RIM)

    def put(index, at, value):
        way, hops, q = firsts[index]
        if way == OURS:
            send[hops, 0, q, at] = value.astype(BF16)
        else:
            start[hops, q, at] = value.astype(BF16)

    def late_part(index):
        way, hops, q = firsts[index]
        slot, ch = slot_of(way, hops), channel(way, q)
        chosen, full = filtered(slot, ch)
        top[index] = full[:RIM]
        put(index, late_span, jnp.dot(full[RIM:].astype(BF16), steering(slot, ch), preferred_element_type=F32))

    def early_part(index):
        way, hops, q = firsts[index]
        slot, ch = slot_of(way, hops), channel(way, q)
        chosen = sets[0, block_of(slot) * per + ch]
        early = with_rim(slot, ch, chosen, top[index]).astype(BF16)
        put(index, early_span, jnp.dot(early, steering(slot, ch), preferred_element_type=F32))

    def leave(index, span):
        way, hops, q = firsts[index]

        @pl.when(length(way, hops, q) == hops)
        def _():
            if way == OURS:
                pass_copy(hops, 0, q, span).start()
            else:
                start_copy(hops, q, span).start()

    load(0, 0).wait()
    load(0, 1).wait()
    for index in range(2 * half):
        late_part(index)
    pl.semaphore_wait(barrier, greeters)

    @pl.when(me == ring - 1)
    def _():
        pl.semaphore_signal(wrap_in, inc=1, device_id={"station": right, "chan": 1}, device_id_type=MESH)

    for index in range(2 * half):
        leave(index, late_span)
    for part in (0, 1):
        send_rim(0, part)
    for slot, part in ((1, partner), (2, core)):
        load(slot, 0).wait()
        send_rim(slot, part)
    for slot in (1, 2):
        load(slot, 1).wait()
    for index in range(2 * half, 4 * half):
        late_part(index)
        leave(index, late_span)
    for slot in range(3, ring):
        start_loads(slot)
    for slot, part in ((1, core), (2, partner)):
        send_rim(slot, part)
    for part in (0, 1):
        wait_rim(0, part)
    for index in range(2 * half):
        early_part(index)
        leave(index, early_span)
    for slot, part in ((1, partner), (2, core)):
        wait_rim(slot, part)
    for index in range(2 * half, 4 * half):
        early_part(index)
        leave(index, early_span)

    def prepare(slot):
        load(slot, 0).wait()
        for part in (0, 1):
            send_rim(slot, part)

    def fill(slots):
        for slot in slots:
            load(slot, 1).wait()
            for part in (0, 1):
                wait_rim(slot, part)

    def term(hops, q):
        reached = length(OURS, hops, q)
        needed = reached > hops
        if not isinstance(hops, int) or hops >= middle - 1:
            begins = jnp.logical_and(reached == hops, jnp.logical_not(is_first(hops, q)))
            needed = jnp.logical_or(needed, begins)

        @pl.when(needed)
        def _():
            own[hops, q] = beams(slot_of(OURS, hops), channel(OURS, q))

        reached = length(THEIRS, hops, q)

        @pl.when(reached > hops)
        def _():
            give[hops, q] = beams(slot_of(THEIRS, hops), channel(THEIRS, q))
            give_copy(hops, q).start()

        @pl.when(jnp.logical_and(reached == hops, jnp.logical_not(is_first(hops, q))))
        def _():
            start[hops, q] = beams(slot_of(THEIRS, hops), channel(THEIRS, q)).astype(BF16)
            start_copy(hops, q).start()

    order = [(q + half) % per for q in range(per)]
    prepare(3)
    prepare(4)
    for slot, part in ((1, core), (2, partner)):
        wait_rim(slot, part)

    @pl.loop(0, CUT + 1)
    def _(step):
        for q in order:
            term(furthest - step, q)

    prepare(5)
    prepare(6)

    def running(hops, rel, q):
        pass_copy(hops + 1, rel, q).wait_recv()
        if rel:
            give_copy(hops, q).wait_recv()
            term_here = lent[hops, q]
        else:
            term_here = own[hops, q]
        send[hops, rel, q] = (term_here + recv[hops + 1, rel, q].astype(F32)).astype(BF16)

    def pass_on(hops, q):
        reached = length(OURS, hops, q)

        @pl.when(jnp.logical_and(reached == hops, jnp.logical_not(is_first(hops, q))))
        def _():
            send[hops, 0, q] = own[hops, q].astype(BF16)
            pass_copy(hops, 0, q).start()

        @pl.when(reached > hops)
        def _():
            for rel in (0, 1):
                running(hops, rel, q)
                pass_copy(hops, rel, q).start()

    @pl.loop(0, furthest - 1)
    def _(step):
        hops = furthest - step
        coming = jnp.maximum(hops - 1, 1)
        more = hops < middle

        @pl.when(jnp.logical_and(first_left, hops == middle - CUT))
        def _():
            pl.semaphore_wait(wrap_in, 2)

        for index, q in enumerate(order):
            pass_on(hops, q)

            @pl.when(more)
            def _():
                if index == 0:
                    fill([slot_of(way, coming) for way in (OURS, THEIRS)])
                term(coming, q)

        @pl.when(jnp.logical_and(more, hops >= 4))
        def _():
            for way in (OURS, THEIRS):
                prepare(slot_of(way, jnp.maximum(hops - 3, 1)))

        @pl.when(hops == 3)
        def _():
            prepare(ring - 1)

    for index, q in enumerate(order):
        for rel in (0, 1):
            running(1, rel, q)
            last_copy(core, rel, q).start()
        if index == 0:
            fill((ring - 1,))
        own[0, q] = beams(ring - 1, q)

    for index, q in enumerate(order):
        for way in (0, 1):
            ch = (q + way * half) % per
            last_copy(way, 0, q).wait_recv()
            total = own[0, ch] + last[way, q].astype(F32)
            if index < half:
                own[0, ch] = total
            else:
                out[ch] = total.T.astype(BF16)

    @pl.loop(1, furthest + 1)
    def _(hops):
        for q in range(per):
            reached = length(OURS, hops, q)

            @pl.when(reached >= hops)
            def _():
                pass_copy(hops, 0, q).wait_send()

            @pl.when(reached > hops)
            def _():
                pass_copy(hops, 1, q).wait_send()

            reached = length(THEIRS, hops, q)

            @pl.when(reached == hops)
            def _():
                start_copy(hops, q).wait_send()

            @pl.when(reached > hops)
            def _():
                give_copy(hops, q).wait_send()

    @pl.when(block < blocks - 1)
    def _():
        @pl.loop(0, ring)
        def _(slot):
            for part in (0, 1):
                rim_copy(slot, part).wait_send()


def body(ring, blocks, voltages, delays, tap_sets, tap_table, weights):
    _, channels, parts, antennas, time = voltages.shape
    beams = weights.shape[-1]
    per = channels // ring
    rows = parts * antennas
    hops = ring // 2 + CUT
    set_count = tap_table.shape[0]
    out = pl.pallas_call(
        functools.partial(kernel, ring, blocks),
        out_shape=jax.ShapeDtypeStruct((per, 2 * beams, time), BF16),
        in_specs=[
            pl.BlockSpec(memory_space=pltpu.HBM),
            pl.BlockSpec(memory_space=pltpu.HBM),
            pl.BlockSpec(memory_space=pltpu.HBM),
            pl.BlockSpec(memory_space=pltpu.SMEM),
            pl.BlockSpec(memory_space=pltpu.HBM),
        ],
        out_specs=pl.BlockSpec(memory_space=pltpu.VMEM),
        scratch_shapes=[
            pltpu.SMEM(tap_sets.shape, jnp.int32),
            pltpu.VMEM(tap_table.shape, BF16),
            pltpu.VMEM((ring, per, rows, time), BF16),
            pltpu.VMEM((ring, per, rows, beams), BF16),
            pltpu.VMEM((ring, per, RIM, rows), BF16),
            pltpu.VMEM((ring, per, RIM, rows), BF16),
            pltpu.VMEM((set_count, time, time), BF16),
            pltpu.VMEM((set_count, RIM, RIM), BF16),
            pltpu.VMEM((2 * per, RIM, rows), F32),
            pltpu.VMEM((hops, per, time, 2 * beams), F32),
            pltpu.VMEM((hops, per, time, 2 * beams), F32),
            pltpu.VMEM((hops, per, time, 2 * beams), F32),
            pltpu.VMEM((hops, 2, per, time, 2 * beams), BF16),
            pltpu.VMEM((hops, per, time, 2 * beams), BF16),
            pltpu.VMEM((hops, 2, per, time, 2 * beams), BF16),
            pltpu.VMEM((2, per, time, 2 * beams), BF16),
            pltpu.SemaphoreType.DMA((2,)),
            pltpu.SemaphoreType.DMA((ring, 2)),
            pltpu.SemaphoreType.DMA((ring, 2)),
            pltpu.SemaphoreType.DMA((ring, 2)),
            pltpu.SemaphoreType.DMA((hops, 2, per)),
            pltpu.SemaphoreType.DMA((hops, per)),
            pltpu.SemaphoreType.DMA((hops, 2, per)),
            pltpu.SemaphoreType.DMA((2, per)),
            pltpu.SemaphoreType.DMA((hops, per)),
            pltpu.SemaphoreType.DMA((hops, per)),
            pltpu.SemaphoreType.REGULAR,
        ],
        compiler_params=pltpu.CompilerParams(
            collective_id=0, has_side_effects=True, vmem_limit_bytes=63 * 1024 * 1024
        ),
    )(
        voltages.reshape(channels, rows, time),
        weights.reshape(channels, rows, beams),
        tap_sets,
        delays,
        tap_table,
    )
    return out.reshape(per, 2, beams, time)


def solution(mesh):
    return jax.shard_map(
        functools.partial(body, mesh.shape["station"], mesh.shape["tm"]),
        mesh=mesh,
        in_specs=(
            P(("group", "station"), "chan", None, None, "tm"),
            P(("group", "station")),
            P(("group", "station"), "chan"),
            P(),
            P(("group", "station"), "chan", None, None, None),
        ),
        out_specs=P(("group", "chan", "station"), None, None, "tm"),
        check_vma=False,
    )
```

```python
import functools

import jax
import jax.numpy as jnp
from jax import lax
from jax.experimental import pallas as pl
from jax.experimental.pallas import tpu as pltpu
from jax.sharding import PartitionSpec as P

TAPS = 16
MAXD = 16
RIM = 32
MESH = pl.DeviceIdType.MESH
F32 = jnp.float32
BF16 = jnp.bfloat16


RIGHT, LEFT = 0, 1


def dot_nt(left, right):
    return lax.dot_general(left, right, (((1,), (1,)), ((), ())), preferred_element_type=F32)


def kernel(
    ring,
    blocks,
    volt,
    steer,
    sets_hbm,
    delays,
    taps_hbm,
    out,
    sets,
    taps,
    vbuf,
    wbuf,
    rim_out,
    rim_in,
    band,
    band_rim,
    top,
    own,
    send,
    recv,
    small_sem,
    load_sem,
    rim_send,
    rim_recv,
    ring_send,
    ring_recv,
):
    me = lax.axis_index("station")
    block = lax.axis_index("tm")
    per = vbuf.shape[1]
    time = vbuf.shape[3]
    rows = vbuf.shape[2]
    antennas = rows // 2
    set_count = taps.shape[0]
    middle, half = ring // 2, per // 2
    sides = (lax.rem(me + 1, ring), lax.rem(me + ring - 1, ring))

    barrier = pltpu.get_barrier_semaphore()
    for side in sides:
        pl.semaphore_signal(barrier, inc=1, device_id={"station": side}, device_id_type=MESH)

    @pl.when(block > 0)
    def _():
        pl.semaphore_signal(barrier, inc=1, device_id={"tm": block - 1}, device_id_type=MESH)

    @pl.when(block < blocks - 1)
    def _():
        pl.semaphore_signal(barrier, inc=1, device_id={"tm": block + 1}, device_id_type=MESH)

    def reach(way, ch):
        right = middle - ch // half
        return right if way == RIGHT else ring - 1 - right

    def slot_of(way, hops):
        nearer = middle - hops
        near = 2 * nearer - 1 if way == RIGHT else 2 * nearer
        return max(near, 0) if isinstance(hops, int) else jnp.maximum(near, 0)

    def block_of(slot):
        odd = slot % 2
        distance = jnp.where(odd == 1, ring - (slot + 1) // 2, slot // 2)
        return lax.rem(me + middle + distance, ring)

    def load(slot, which):
        source, target = ((volt, vbuf), (steer, wbuf))[which]
        at = block_of(slot) * per
        return pltpu.make_async_copy(source.at[pl.ds(at, per)], target.at[slot], load_sem.at[slot, which])

    def start_loads(slot):
        load(slot, 0).start()
        load(slot, 1).start()

    small = [
        pltpu.make_async_copy(source, target, small_sem.at[index])
        for index, (source, target) in enumerate(((taps_hbm, taps), (sets_hbm, sets)))
    ]
    for copy in small:
        copy.start()
    for slot in range(3):
        start_loads(slot)
    for copy in small:
        copy.wait()

    delay = delays[0]
    table = taps[...].astype(F32)
    lane = lax.broadcasted_iota(jnp.int32, (set_count, time), 1)
    base = jnp.zeros((set_count, time), F32)
    for tap in range(TAPS):
        base = jnp.where((lane + (tap + delay)) % time == 0, table[:, tap : tap + 1], base)
    row_at = lax.broadcasted_iota(jnp.int32, (time, time), 0)
    col_at = lax.broadcasted_iota(jnp.int32, (time, time), 1)
    for index in range(set_count):
        spread = jnp.broadcast_to(base[index : index + 1], (time, time))
        turned = pltpu.roll(spread, 0, 1, stride=1, stride_axis=0)
        band[index] = jnp.where(col_at <= row_at, turned, 0.0).astype(BF16)
        turned = pltpu.roll(spread[:RIM], RIM, 1, stride=1, stride_axis=0)
        band_rim[index] = turned[:, :RIM].astype(BF16)

    pick_row = lax.broadcasted_iota(jnp.int32, (RIM, time), 0)
    pick_col = lax.broadcasted_iota(jnp.int32, (RIM, time), 1)
    pick = jnp.where(pick_col == pick_row + (time - RIM), 1.0, 0.0).astype(BF16)

    def rim_copy(slot, part):
        pair = pl.ds(part * half, half)
        return pltpu.make_async_remote_copy(
            src_ref=rim_out.at[slot, pair],
            dst_ref=rim_in.at[slot, pair],
            send_sem=rim_send.at[slot, part],
            recv_sem=rim_recv.at[slot, part],
            device_id={"tm": lax.rem(block + 1, blocks)},
            device_id_type=MESH,
        )

    def send_rim(slot, part):
        @pl.when(block < blocks - 1)
        def _():
            for ch in range(part * half, (part + 1) * half):
                rim_out[slot, ch] = dot_nt(pick, vbuf[slot, ch]).astype(BF16)
            rim_copy(slot, part).start()

    def wait_rim(slot, part):
        @pl.when(block > 0)
        def _():
            rim_copy(slot, part).wait_recv()

    @pl.when(block == 0)
    def _():
        rim_in[...] = jnp.zeros_like(rim_in)

    def steering(slot, ch):
        real_w = wbuf[slot, ch, :antennas]
        imag_w = wbuf[slot, ch, antennas:]
        upper = jnp.concatenate([real_w, imag_w], axis=1)
        lower = jnp.concatenate([-imag_w, real_w], axis=1)
        return jnp.concatenate([upper, lower], axis=0)

    def filtered(slot, ch):
        chosen = sets[0, block_of(slot) * per + ch]
        return chosen, dot_nt(band[chosen], vbuf[slot, ch])

    def with_rim(slot, ch, chosen, early):
        return early + jnp.dot(band_rim[chosen], rim_in[slot, ch], preferred_element_type=F32)

    def beams(slot, ch):
        chosen, full = filtered(slot, ch)
        early = with_rim(slot, ch, chosen, full[:RIM])
        delayed = jnp.concatenate([early, full[RIM:]], axis=0).astype(BF16)
        return jnp.dot(delayed, steering(slot, ch), preferred_element_type=F32)

    def ring_copy(way, hops, ch, part=None):
        span = pl.ds(0, time) if part is None else part
        return pltpu.make_async_remote_copy(
            src_ref=send.at[way, hops, ch, span],
            dst_ref=recv.at[way, hops, ch, span],
            send_sem=ring_send.at[way, hops, ch],
            recv_sem=ring_recv.at[way, hops, ch],
            device_id={"station": sides[way]},
            device_id_type=MESH,
        )

    firsts = []
    for back in (0, 1):
        for q in range(half):
            firsts.append((RIGHT, middle - back, back * half + q))
            firsts.append((LEFT, middle - back, (1 - back) * half + q))
    early_span, late_span = pl.ds(0, RIM), pl.ds(RIM, time - RIM)

    def late_part(index):
        way, hops, ch = firsts[index]
        slot = slot_of(way, hops)
        chosen, full = filtered(slot, ch)
        top[index] = full[:RIM]
        late = jnp.dot(full[RIM:].astype(BF16), steering(slot, ch), preferred_element_type=F32)
        send[way, hops, ch, RIM:] = late.astype(BF16)

    def early_part(index):
        way, hops, ch = firsts[index]
        slot = slot_of(way, hops)
        chosen = sets[0, block_of(slot) * per + ch]
        early = with_rim(slot, ch, chosen, top[index]).astype(BF16)
        early = jnp.dot(early, steering(slot, ch), preferred_element_type=F32)
        send[way, hops, ch, :RIM] = early.astype(BF16)

    def leave(index, span):
        way, hops, ch = firsts[index]
        ring_copy(way, hops, ch, span).start()

    load(0, 0).wait()
    load(0, 1).wait()
    for index in range(2 * half):
        late_part(index)
    greeters = 2 + jnp.where(block > 0, 1, 0) + jnp.where(block < blocks - 1, 1, 0)
    pl.semaphore_wait(barrier, greeters)
    for index in range(2 * half):
        leave(index, late_span)
    for part in (0, 1):
        send_rim(0, part)
    for slot in (1, 2):
        load(slot, 0).wait()
        send_rim(slot, 2 - slot)
    for slot in (1, 2):
        load(slot, 1).wait()
    for index in range(2 * half, 4 * half):
        late_part(index)
        leave(index, late_span)
    for slot in range(3, ring):
        start_loads(slot)
    for slot in (1, 2):
        send_rim(slot, slot - 1)
    for part in (0, 1):
        wait_rim(0, part)
    for index in range(2 * half):
        early_part(index)
        leave(index, early_span)
    for slot in (1, 2):
        wait_rim(slot, 2 - slot)
    for index in range(2 * half, 4 * half):
        early_part(index)
        leave(index, early_span)

    def prepare(slot):
        load(slot, 0).wait()
        for part in (0, 1):
            send_rim(slot, part)

    def fill(slots):
        for slot in slots:
            load(slot, 1).wait()
            for part in (0, 1):
                wait_rim(slot, part)

    prepare(3)
    prepare(4)
    for slot in (1, 2):
        wait_rim(slot, slot - 1)
    for ch in range(half):
        own[1, ch] = beams(1, ch)
        own[2, ch + half] = beams(2, ch + half)
    prepare(5)
    prepare(6)

    order = ([(q + half) % per for q in range(per)], list(range(per)))

    def pass_on(way, hops, ch):
        slot = slot_of(way, hops)

        @pl.when(reach(way, ch) > hops)
        def _():
            ring_copy(way, hops + 1, ch).wait_recv()
            total = own[slot, ch] + recv[way, hops + 1, ch].astype(F32)
            send[way, hops, ch] = total.astype(BF16)
            ring_copy(way, hops, ch).start()

    @pl.loop(1, middle)
    def _(step):
        hops = middle - step
        coming = hops - 1
        slots = [slot_of(way, jnp.maximum(coming, 1)) for way in (RIGHT, LEFT)]

        for q in range(per):
            pass_on(LEFT, hops, order[LEFT][q])
            pass_on(RIGHT, hops, order[RIGHT][q])

        @pl.when(coming >= 1)
        def _():
            fill(slots)
            for q in range(per):
                for way in (RIGHT, LEFT):
                    ch = order[way][q]
                    own[slots[way], ch] = beams(slots[way], ch)

        @pl.when(coming == 0)
        def _():
            fill((ring - 1,))
            for q in range(per):
                own[ring - 1, q] = beams(ring - 1, q)

        @pl.when(coming >= 3)
        def _():
            for way in (RIGHT, LEFT):
                prepare(slot_of(way, jnp.maximum(coming - 2, 1)))

        @pl.when(coming == 2)
        def _():
            prepare(ring - 1)

    for q in range(per):
        for way in (RIGHT, LEFT):
            ch = order[way][q]
            ring_copy(way, 1, ch).wait_recv()
            total = own[ring - 1, ch] + recv[way, 1, ch].astype(F32)
            if q < half:
                own[ring - 1, ch] = total
            else:
                out[ch] = total.T.astype(BF16)

    @pl.loop(1, middle + 1)
    def _(hops):
        for way in (RIGHT, LEFT):
            for ch in range(per):

                @pl.when(reach(way, ch) >= hops)
                def _():
                    ring_copy(way, hops, ch).wait_send()

    @pl.when(block < blocks - 1)
    def _():
        @pl.loop(0, ring)
        def _(slot):
            for part in (0, 1):
                rim_copy(slot, part).wait_send()


def body(ring, blocks, voltages, delays, tap_sets, tap_table, weights):
    _, channels, parts, antennas, time = voltages.shape
    beams = weights.shape[-1]
    per = channels // ring
    rows = parts * antennas
    hops = ring // 2 + 1
    set_count = tap_table.shape[0]
    out = pl.pallas_call(
        functools.partial(kernel, ring, blocks),
        out_shape=jax.ShapeDtypeStruct((per, 2 * beams, time), BF16),
        in_specs=[
            pl.BlockSpec(memory_space=pltpu.HBM),
            pl.BlockSpec(memory_space=pltpu.HBM),
            pl.BlockSpec(memory_space=pltpu.HBM),
            pl.BlockSpec(memory_space=pltpu.SMEM),
            pl.BlockSpec(memory_space=pltpu.HBM),
        ],
        out_specs=pl.BlockSpec(memory_space=pltpu.VMEM),
        scratch_shapes=[
            pltpu.SMEM(tap_sets.shape, jnp.int32),
            pltpu.VMEM(tap_table.shape, BF16),
            pltpu.VMEM((ring, per, rows, time), BF16),
            pltpu.VMEM((ring, per, rows, beams), BF16),
            pltpu.VMEM((ring, per, RIM, rows), BF16),
            pltpu.VMEM((ring, per, RIM, rows), BF16),
            pltpu.VMEM((set_count, time, time), BF16),
            pltpu.VMEM((set_count, RIM, RIM), BF16),
            pltpu.VMEM((2 * per, RIM, rows), F32),
            pltpu.VMEM((ring, per, time, 2 * beams), F32),
            pltpu.VMEM((2, hops, per, time, 2 * beams), BF16),
            pltpu.VMEM((2, hops, per, time, 2 * beams), BF16),
            pltpu.SemaphoreType.DMA((2,)),
            pltpu.SemaphoreType.DMA((ring, 2)),
            pltpu.SemaphoreType.DMA((ring, 2)),
            pltpu.SemaphoreType.DMA((ring, 2)),
            pltpu.SemaphoreType.DMA((2, hops, per)),
            pltpu.SemaphoreType.DMA((2, hops, per)),
        ],
        compiler_params=pltpu.CompilerParams(
            collective_id=0, has_side_effects=True, vmem_limit_bytes=63 * 1024 * 1024
        ),
    )(
        voltages.reshape(channels, rows, time),
        weights.reshape(channels, rows, beams),
        tap_sets,
        delays,
        tap_table,
    )
    return out.reshape(per, 2, beams, time)


def solution(mesh):
    return jax.shard_map(
        functools.partial(body, mesh.shape["station"], mesh.shape["tm"]),
        mesh=mesh,
        in_specs=(
            P(("group", "station"), "chan", None, None, "tm"),
            P(("group", "station")),
            P(("group", "station"), "chan"),
            P(),
            P(("group", "station"), "chan", None, None, None),
        ),
        out_specs=P(("group", "chan", "station"), None, None, "tm"),
        check_vma=False,
    )
```

```python
import functools

import jax
import jax.numpy as jnp
from jax import lax
from jax.experimental import pallas as pl
from jax.experimental.pallas import tpu as pltpu
from jax.sharding import PartitionSpec as P

TAPS = 16
MAXD = 16
RIM = 32
MESH = pl.DeviceIdType.MESH
F32 = jnp.float32
BF16 = jnp.bfloat16


RIGHT, LEFT = 0, 1
PIECES = 2


def dot_nt(left, right):
    return lax.dot_general(left, right, (((1,), (1,)), ((), ())), preferred_element_type=F32)


def kernel(
    ring,
    blocks,
    volt,
    steer,
    sets_hbm,
    delays,
    taps_hbm,
    out,
    sets,
    taps,
    vbuf,
    wbuf,
    rim_out,
    rim_in,
    band,
    band_rim,
    top,
    own,
    send,
    recv,
    small_sem,
    load_sem,
    rim_send,
    rim_recv,
    ring_send,
    ring_recv,
):
    me = lax.axis_index("station")
    block = lax.axis_index("tm")
    per = vbuf.shape[1]
    time = vbuf.shape[3]
    rows = vbuf.shape[2]
    antennas = rows // 2
    set_count = taps.shape[0]
    middle, half = ring // 2, per // 2
    rows_sent = time // PIECES
    sides = (lax.rem(me + 1, ring), lax.rem(me + ring - 1, ring))

    barrier = pltpu.get_barrier_semaphore()
    for side in sides:
        pl.semaphore_signal(barrier, inc=1, device_id={"station": side}, device_id_type=MESH)

    @pl.when(block > 0)
    def _():
        pl.semaphore_signal(barrier, inc=1, device_id={"tm": block - 1}, device_id_type=MESH)

    @pl.when(block < blocks - 1)
    def _():
        pl.semaphore_signal(barrier, inc=1, device_id={"tm": block + 1}, device_id_type=MESH)

    def reach(way, ch):
        right = middle - ch // half
        return right if way == RIGHT else ring - 1 - right

    def slot_of(way, hops):
        nearer = middle - hops
        near = 2 * nearer - 1 if way == RIGHT else 2 * nearer
        return max(near, 0) if isinstance(hops, int) else jnp.maximum(near, 0)

    def block_of(slot):
        odd = slot % 2
        distance = jnp.where(odd == 1, ring - (slot + 1) // 2, slot // 2)
        return lax.rem(me + middle + distance, ring)

    def load(slot, which):
        source, target = ((volt, vbuf), (steer, wbuf))[which]
        at = block_of(slot) * per
        return pltpu.make_async_copy(source.at[pl.ds(at, per)], target.at[slot], load_sem.at[slot, which])

    def start_loads(slot):
        load(slot, 0).start()
        load(slot, 1).start()

    small = [
        pltpu.make_async_copy(source, target, small_sem.at[index])
        for index, (source, target) in enumerate(((taps_hbm, taps), (sets_hbm, sets)))
    ]
    for copy in small:
        copy.start()
    for slot in range(3):
        start_loads(slot)
    for copy in small:
        copy.wait()

    delay = delays[0]
    table = taps[...].astype(F32)
    lane = lax.broadcasted_iota(jnp.int32, (set_count, time), 1)
    base = jnp.zeros((set_count, time), F32)
    for tap in range(TAPS):
        base = jnp.where((lane + (tap + delay)) % time == 0, table[:, tap : tap + 1], base)
    row_at = lax.broadcasted_iota(jnp.int32, (time, time), 0)
    col_at = lax.broadcasted_iota(jnp.int32, (time, time), 1)
    for index in range(set_count):
        spread = jnp.broadcast_to(base[index : index + 1], (time, time))
        turned = pltpu.roll(spread, 0, 1, stride=1, stride_axis=0)
        band[index] = jnp.where(col_at <= row_at, turned, 0.0).astype(BF16)
        turned = pltpu.roll(spread[:RIM], RIM, 1, stride=1, stride_axis=0)
        band_rim[index] = turned[:, :RIM].astype(BF16)

    pick_row = lax.broadcasted_iota(jnp.int32, (RIM, time), 0)
    pick_col = lax.broadcasted_iota(jnp.int32, (RIM, time), 1)
    pick = jnp.where(pick_col == pick_row + (time - RIM), 1.0, 0.0).astype(BF16)

    def rim_copy(slot, part):
        pair = pl.ds(part * half, half)
        return pltpu.make_async_remote_copy(
            src_ref=rim_out.at[slot, pair],
            dst_ref=rim_in.at[slot, pair],
            send_sem=rim_send.at[slot, part],
            recv_sem=rim_recv.at[slot, part],
            device_id={"tm": lax.rem(block + 1, blocks)},
            device_id_type=MESH,
        )

    def send_rim(slot, part):
        @pl.when(block < blocks - 1)
        def _():
            for ch in range(part * half, (part + 1) * half):
                rim_out[slot, ch] = dot_nt(pick, vbuf[slot, ch]).astype(BF16)
            rim_copy(slot, part).start()

    def wait_rim(slot, part):
        @pl.when(block > 0)
        def _():
            rim_copy(slot, part).wait_recv()

    @pl.when(block == 0)
    def _():
        rim_in[...] = jnp.zeros_like(rim_in)

    def steering(slot, ch):
        real_w = wbuf[slot, ch, :antennas]
        imag_w = wbuf[slot, ch, antennas:]
        upper = jnp.concatenate([real_w, imag_w], axis=1)
        lower = jnp.concatenate([-imag_w, real_w], axis=1)
        return jnp.concatenate([upper, lower], axis=0)

    def filtered(slot, ch):
        chosen = sets[0, block_of(slot) * per + ch]
        return chosen, dot_nt(band[chosen], vbuf[slot, ch])

    def with_rim(slot, ch, chosen, early):
        return early + jnp.dot(band_rim[chosen], rim_in[slot, ch], preferred_element_type=F32)

    def beams(slot, ch):
        chosen, full = filtered(slot, ch)
        early = with_rim(slot, ch, chosen, full[:RIM])
        delayed = jnp.concatenate([early, full[RIM:]], axis=0).astype(BF16)
        return jnp.dot(delayed, steering(slot, ch), preferred_element_type=F32)

    def ring_copy(way, hops, ch, piece, part=None):
        span = pl.ds(piece * rows_sent, rows_sent) if part is None else part
        return pltpu.make_async_remote_copy(
            src_ref=send.at[way, hops, ch, span],
            dst_ref=recv.at[way, hops, ch, span],
            send_sem=ring_send.at[way, hops, ch, piece],
            recv_sem=ring_recv.at[way, hops, ch, piece],
            device_id={"station": sides[way]},
            device_id_type=MESH,
        )

    firsts = []
    for back in (0, 1):
        for q in range(half):
            firsts.append((RIGHT, middle - back, back * half + q))
            firsts.append((LEFT, middle - back, (1 - back) * half + q))

    def late_part(index):
        way, hops, ch = firsts[index]
        slot = slot_of(way, hops)
        chosen, full = filtered(slot, ch)
        top[index] = full[:RIM]
        late = jnp.dot(full[RIM:].astype(BF16), steering(slot, ch), preferred_element_type=F32)
        send[way, hops, ch, RIM:] = late.astype(BF16)

    def early_part(index):
        way, hops, ch = firsts[index]
        slot = slot_of(way, hops)
        chosen = sets[0, block_of(slot) * per + ch]
        early = with_rim(slot, ch, chosen, top[index]).astype(BF16)
        early = jnp.dot(early, steering(slot, ch), preferred_element_type=F32)
        send[way, hops, ch, :RIM] = early.astype(BF16)

    def leave_late(index):
        way, hops, ch = firsts[index]
        for piece in range(1, PIECES):
            ring_copy(way, hops, ch, piece).start()
        ring_copy(way, hops, ch, 0, pl.ds(RIM, rows_sent - RIM)).start()

    def leave_early(index):
        way, hops, ch = firsts[index]
        ring_copy(way, hops, ch, 0, pl.ds(0, RIM)).start()

    load(0, 0).wait()
    load(0, 1).wait()
    greeters = 2 + jnp.where(block > 0, 1, 0) + jnp.where(block < blocks - 1, 1, 0)
    pl.semaphore_wait(barrier, greeters)
    for index in range(2 * half):
        late_part(index)
        leave_late(index)
    for part in (0, 1):
        send_rim(0, part)
    for slot in (1, 2):
        load(slot, 0).wait()
        send_rim(slot, 2 - slot)
    for slot in (1, 2):
        load(slot, 1).wait()
    for index in range(2 * half, 4 * half):
        late_part(index)
        leave_late(index)
    for slot in range(3, ring):
        start_loads(slot)
    for slot in (1, 2):
        send_rim(slot, slot - 1)
    for part in (0, 1):
        wait_rim(0, part)
    for index in range(2 * half):
        early_part(index)
        leave_early(index)
    for slot in (1, 2):
        wait_rim(slot, 2 - slot)
    for index in range(2 * half, 4 * half):
        early_part(index)
        leave_early(index)

    def prepare(slot):
        load(slot, 0).wait()
        for part in (0, 1):
            send_rim(slot, part)

    def fill(slots):
        for slot in slots:
            load(slot, 1).wait()
            for part in (0, 1):
                wait_rim(slot, part)

    prepare(3)
    prepare(4)
    for slot in (1, 2):
        wait_rim(slot, slot - 1)
    for ch in range(half):
        own[1, ch] = beams(1, ch)
        own[2, ch + half] = beams(2, ch + half)
    prepare(5)
    prepare(6)

    order = ([(q + half) % per for q in range(per)], list(range(per)))

    pieces = list(range(1, PIECES)) + [0]

    def pass_on(way, hops, ch):
        slot = slot_of(way, hops)

        @pl.when(reach(way, ch) > hops)
        def _():
            for piece in pieces:
                at = pl.ds(piece * rows_sent, rows_sent)
                ring_copy(way, hops + 1, ch, piece).wait_recv()
                total = own[slot, ch, at] + recv[way, hops + 1, ch, at].astype(F32)
                send[way, hops, ch, at] = total.astype(BF16)
                ring_copy(way, hops, ch, piece).start()

    @pl.loop(1, middle)
    def _(step):
        hops = middle - step
        coming = hops - 1
        slots = [slot_of(way, jnp.maximum(coming, 1)) for way in (RIGHT, LEFT)]

        for q in range(per):
            pass_on(LEFT, hops, order[LEFT][q])
            pass_on(RIGHT, hops, order[RIGHT][q])

        @pl.when(coming >= 1)
        def _():
            fill(slots)
            for q in range(per):
                for way in (RIGHT, LEFT):
                    ch = order[way][q]
                    own[slots[way], ch] = beams(slots[way], ch)

        @pl.when(coming == 0)
        def _():
            fill((ring - 1,))
            for q in range(per):
                own[ring - 1, q] = beams(ring - 1, q)

        @pl.when(coming >= 3)
        def _():
            for way in (RIGHT, LEFT):
                prepare(slot_of(way, jnp.maximum(coming - 2, 1)))

        @pl.when(coming == 2)
        def _():
            prepare(ring - 1)

    for q in range(per):
        for way in (RIGHT, LEFT):
            ch = order[way][q]
            for piece in pieces:
                at = pl.ds(piece * rows_sent, rows_sent)
                ring_copy(way, 1, ch, piece).wait_recv()
                total = own[ring - 1, ch, at] + recv[way, 1, ch, at].astype(F32)
                own[ring - 1, ch, at] = total
            if q >= half:
                out[ch] = own[ring - 1, ch].T.astype(BF16)

    @pl.loop(1, middle + 1)
    def _(hops):
        for way in (RIGHT, LEFT):
            for ch in range(per):

                @pl.when(reach(way, ch) >= hops)
                def _():
                    for piece in pieces:
                        ring_copy(way, hops, ch, piece).wait_send()

    @pl.when(block < blocks - 1)
    def _():
        @pl.loop(0, ring)
        def _(slot):
            for part in (0, 1):
                rim_copy(slot, part).wait_send()


def body(ring, blocks, voltages, delays, tap_sets, tap_table, weights):
    _, channels, parts, antennas, time = voltages.shape
    beams = weights.shape[-1]
    per = channels // ring
    rows = parts * antennas
    hops = ring // 2 + 1
    set_count = tap_table.shape[0]
    out = pl.pallas_call(
        functools.partial(kernel, ring, blocks),
        out_shape=jax.ShapeDtypeStruct((per, 2 * beams, time), BF16),
        in_specs=[
            pl.BlockSpec(memory_space=pltpu.HBM),
            pl.BlockSpec(memory_space=pltpu.HBM),
            pl.BlockSpec(memory_space=pltpu.HBM),
            pl.BlockSpec(memory_space=pltpu.SMEM),
            pl.BlockSpec(memory_space=pltpu.HBM),
        ],
        out_specs=pl.BlockSpec(memory_space=pltpu.VMEM),
        scratch_shapes=[
            pltpu.SMEM(tap_sets.shape, jnp.int32),
            pltpu.VMEM(tap_table.shape, BF16),
            pltpu.VMEM((ring, per, rows, time), BF16),
            pltpu.VMEM((ring, per, rows, beams), BF16),
            pltpu.VMEM((ring, per, RIM, rows), BF16),
            pltpu.VMEM((ring, per, RIM, rows), BF16),
            pltpu.VMEM((set_count, time, time), BF16),
            pltpu.VMEM((set_count, RIM, RIM), BF16),
            pltpu.VMEM((2 * per, RIM, rows), F32),
            pltpu.VMEM((ring, per, time, 2 * beams), F32),
            pltpu.VMEM((2, hops, per, time, 2 * beams), BF16),
            pltpu.VMEM((2, hops, per, time, 2 * beams), BF16),
            pltpu.SemaphoreType.DMA((2,)),
            pltpu.SemaphoreType.DMA((ring, 2)),
            pltpu.SemaphoreType.DMA((ring, 2)),
            pltpu.SemaphoreType.DMA((ring, 2)),
            pltpu.SemaphoreType.DMA((2, hops, per, PIECES)),
            pltpu.SemaphoreType.DMA((2, hops, per, PIECES)),
        ],
        compiler_params=pltpu.CompilerParams(
            collective_id=0, has_side_effects=True, vmem_limit_bytes=63 * 1024 * 1024
        ),
    )(
        voltages.reshape(channels, rows, time),
        weights.reshape(channels, rows, beams),
        tap_sets,
        delays,
        tap_table,
    )
    return out.reshape(per, 2, beams, time)


def solution(mesh):
    return jax.shard_map(
        functools.partial(body, mesh.shape["station"], mesh.shape["tm"]),
        mesh=mesh,
        in_specs=(
            P(("group", "station"), "chan", None, None, "tm"),
            P(("group", "station")),
            P(("group", "station"), "chan"),
            P(),
            P(("group", "station"), "chan", None, None, None),
        ),
        out_specs=P(("group", "chan", "station"), None, None, "tm"),
        check_vma=False,
    )
```

```python
import functools

import jax
import jax.numpy as jnp
from jax import lax
from jax.experimental import pallas as pl
from jax.experimental.pallas import tpu as pltpu
from jax.sharding import PartitionSpec as P

TAPS = 16
MAXD = 16
RIM = 32
MESH = pl.DeviceIdType.MESH
F32 = jnp.float32
BF16 = jnp.bfloat16


RIGHT, LEFT = 0, 1


def dot_nt(left, right):
    return lax.dot_general(left, right, (((1,), (1,)), ((), ())), preferred_element_type=F32)


def kernel(
    ring,
    blocks,
    volt,
    steer,
    sets_hbm,
    delays,
    taps_hbm,
    out,
    sets,
    taps,
    vbuf,
    wbuf,
    rim_out,
    rim_in,
    band,
    band_rim,
    top,
    own,
    send,
    recv,
    small_sem,
    load_sem,
    rim_send,
    rim_recv,
    ring_send,
    ring_recv,
):
    me = lax.axis_index("station")
    block = lax.axis_index("tm")
    per = vbuf.shape[1]
    time = vbuf.shape[3]
    rows = vbuf.shape[2]
    antennas = rows // 2
    set_count = taps.shape[0]
    middle, half = ring // 2, per // 2
    sides = (lax.rem(me + 1, ring), lax.rem(me + ring - 1, ring))

    barrier = pltpu.get_barrier_semaphore()
    for side in sides:
        pl.semaphore_signal(barrier, inc=1, device_id={"station": side}, device_id_type=MESH)

    @pl.when(block > 0)
    def _():
        pl.semaphore_signal(barrier, inc=1, device_id={"tm": block - 1}, device_id_type=MESH)

    @pl.when(block < blocks - 1)
    def _():
        pl.semaphore_signal(barrier, inc=1, device_id={"tm": block + 1}, device_id_type=MESH)

    def reach(way, ch):
        right = middle - ch // half
        return right if way == RIGHT else ring - 1 - right

    def slot_of(way, hops):
        nearer = middle - hops
        near = 2 * nearer - 1 if way == RIGHT else 2 * nearer
        return max(near, 0) if isinstance(hops, int) else jnp.maximum(near, 0)

    def block_of(slot):
        odd = slot % 2
        distance = jnp.where(odd == 1, ring - (slot + 1) // 2, slot // 2)
        return lax.rem(me + middle + distance, ring)

    def load(slot, which):
        source, target = ((volt, vbuf), (steer, wbuf))[which]
        at = block_of(slot) * per
        return pltpu.make_async_copy(source.at[pl.ds(at, per)], target.at[slot], load_sem.at[slot, which])

    def start_loads(slot):
        load(slot, 0).start()
        load(slot, 1).start()

    small = [
        pltpu.make_async_copy(source, target, small_sem.at[index])
        for index, (source, target) in enumerate(((taps_hbm, taps), (sets_hbm, sets)))
    ]
    for copy in small:
        copy.start()
    for slot in range(3):
        start_loads(slot)
    for copy in small:
        copy.wait()

    delay = delays[0]
    table = taps[...].astype(F32)
    lane = lax.broadcasted_iota(jnp.int32, (set_count, time), 1)
    base = jnp.zeros((set_count, time), F32)
    for tap in range(TAPS):
        base = jnp.where((lane + (tap + delay)) % time == 0, table[:, tap : tap + 1], base)
    row_at = lax.broadcasted_iota(jnp.int32, (time, time), 0)
    col_at = lax.broadcasted_iota(jnp.int32, (time, time), 1)
    for index in range(set_count):
        spread = jnp.broadcast_to(base[index : index + 1], (time, time))
        turned = pltpu.roll(spread, 0, 1, stride=1, stride_axis=0)
        band[index] = jnp.where(col_at <= row_at, turned, 0.0).astype(BF16)
        turned = pltpu.roll(spread[:RIM], RIM, 1, stride=1, stride_axis=0)
        band_rim[index] = turned[:, :RIM].astype(BF16)

    pick_row = lax.broadcasted_iota(jnp.int32, (RIM, time), 0)
    pick_col = lax.broadcasted_iota(jnp.int32, (RIM, time), 1)
    pick = jnp.where(pick_col == pick_row + (time - RIM), 1.0, 0.0).astype(BF16)

    def rim_copy(slot, part):
        pair = pl.ds(part * half, half)
        return pltpu.make_async_remote_copy(
            src_ref=rim_out.at[slot, pair],
            dst_ref=rim_in.at[slot, pair],
            send_sem=rim_send.at[slot, part],
            recv_sem=rim_recv.at[slot, part],
            device_id={"tm": lax.rem(block + 1, blocks)},
            device_id_type=MESH,
        )

    def send_rim(slot, part):
        @pl.when(block < blocks - 1)
        def _():
            for ch in range(part * half, (part + 1) * half):
                rim_out[slot, ch] = dot_nt(pick, vbuf[slot, ch]).astype(BF16)
            rim_copy(slot, part).start()

    def wait_rim(slot, part):
        @pl.when(block > 0)
        def _():
            rim_copy(slot, part).wait_recv()

    @pl.when(block == 0)
    def _():
        rim_in[...] = jnp.zeros_like(rim_in)

    def steering(slot, ch):
        real_w = wbuf[slot, ch, :antennas]
        imag_w = wbuf[slot, ch, antennas:]
        upper = jnp.concatenate([real_w, imag_w], axis=1)
        lower = jnp.concatenate([-imag_w, real_w], axis=1)
        return jnp.concatenate([upper, lower], axis=0)

    def filtered(slot, ch):
        chosen = sets[0, block_of(slot) * per + ch]
        return chosen, dot_nt(band[chosen], vbuf[slot, ch])

    def with_rim(slot, ch, chosen, early):
        return early + jnp.dot(band_rim[chosen], rim_in[slot, ch], preferred_element_type=F32)

    def beams(slot, ch):
        chosen, full = filtered(slot, ch)
        early = with_rim(slot, ch, chosen, full[:RIM])
        delayed = jnp.concatenate([early, full[RIM:]], axis=0).astype(BF16)
        return jnp.dot(delayed, steering(slot, ch), preferred_element_type=F32)

    def ring_copy(way, hops, ch, part=None):
        span = pl.ds(0, time) if part is None else part
        return pltpu.make_async_remote_copy(
            src_ref=send.at[way, hops, ch, span],
            dst_ref=recv.at[way, hops, ch, span],
            send_sem=ring_send.at[way, hops, ch],
            recv_sem=ring_recv.at[way, hops, ch],
            device_id={"station": sides[way]},
            device_id_type=MESH,
        )

    firsts = []
    for back in (0, 1):
        for q in range(half):
            firsts.append((RIGHT, middle - back, back * half + q))
            firsts.append((LEFT, middle - back, (1 - back) * half + q))
    early_span, late_span = pl.ds(0, RIM), pl.ds(RIM, time - RIM)

    def late_part(index):
        way, hops, ch = firsts[index]
        slot = slot_of(way, hops)
        chosen, full = filtered(slot, ch)
        top[index] = full[:RIM]
        late = jnp.dot(full[RIM:].astype(BF16), steering(slot, ch), preferred_element_type=F32)
        send[way, hops, ch, RIM:] = late.astype(BF16)

    def early_part(index):
        way, hops, ch = firsts[index]
        slot = slot_of(way, hops)
        chosen = sets[0, block_of(slot) * per + ch]
        early = with_rim(slot, ch, chosen, top[index]).astype(BF16)
        early = jnp.dot(early, steering(slot, ch), preferred_element_type=F32)
        send[way, hops, ch, :RIM] = early.astype(BF16)

    def leave(index, span):
        way, hops, ch = firsts[index]
        ring_copy(way, hops, ch, span).start()

    load(0, 0).wait()
    load(0, 1).wait()
    greeters = 2 + jnp.where(block > 0, 1, 0) + jnp.where(block < blocks - 1, 1, 0)
    pl.semaphore_wait(barrier, greeters)
    for index in range(2 * half):
        late_part(index)
        leave(index, late_span)
    for part in (0, 1):
        send_rim(0, part)
    for slot in (1, 2):
        load(slot, 0).wait()
        send_rim(slot, 2 - slot)
    for slot in (1, 2):
        load(slot, 1).wait()
    for index in range(2 * half, 4 * half):
        late_part(index)
        leave(index, late_span)
    for slot in range(3, ring):
        start_loads(slot)
    for slot in (1, 2):
        send_rim(slot, slot - 1)
    for part in (0, 1):
        wait_rim(0, part)
    for index in range(2 * half):
        early_part(index)
        leave(index, early_span)
    for slot in (1, 2):
        wait_rim(slot, 2 - slot)
    for index in range(2 * half, 4 * half):
        early_part(index)
        leave(index, early_span)

    def prepare(slot):
        load(slot, 0).wait()
        for part in (0, 1):
            send_rim(slot, part)

    def fill(slots):
        for slot in slots:
            load(slot, 1).wait()
            for part in (0, 1):
                wait_rim(slot, part)

    prepare(3)
    prepare(4)
    for slot in (1, 2):
        wait_rim(slot, slot - 1)
    for ch in range(half):
        own[1, ch] = beams(1, ch)
        own[2, ch + half] = beams(2, ch + half)
    prepare(5)
    prepare(6)

    order = ([(q + half) % per for q in range(per)], list(range(per)))

    def pass_on(way, hops, ch):
        slot = slot_of(way, hops)

        @pl.when(reach(way, ch) > hops)
        def _():
            ring_copy(way, hops + 1, ch).wait_recv()
            total = own[slot, ch] + recv[way, hops + 1, ch].astype(F32)
            send[way, hops, ch] = total.astype(BF16)
            ring_copy(way, hops, ch).start()

    @pl.loop(1, middle)
    def _(step):
        hops = middle - step
        coming = hops - 1
        slots = [slot_of(way, jnp.maximum(coming, 1)) for way in (RIGHT, LEFT)]

        early = hops == middle - 1
        rims = [slot_of(way, jnp.maximum(coming - 2, 1)) for way in (RIGHT, LEFT)]

        def terms(q):
            for way in (RIGHT, LEFT):
                ch = order[way][q]
                own[slots[way], ch] = beams(slots[way], ch)

        for q in range(per):
            pass_on(LEFT, hops, order[LEFT][q])
            pass_on(RIGHT, hops, order[RIGHT][q])

            @pl.when(jnp.logical_and(coming >= 1, jnp.logical_not(early)))
            def _():
                if q == 0:
                    fill(slots)
                terms(q)

            @pl.when(coming == 0)
            def _():
                if q == 0:
                    fill((ring - 1,))
                own[ring - 1, q] = beams(ring - 1, q)

            @pl.when(coming >= 3)
            def _():
                slot, part = rims[q // 2], q % 2
                if part == 0:
                    load(slot, 0).wait()
                send_rim(slot, part)

        @pl.when(early)
        def _():
            fill(slots)
            for q in range(per):
                terms(q)

        @pl.when(coming == 2)
        def _():
            prepare(ring - 1)

    for q in range(per):
        for way in (RIGHT, LEFT):
            ch = order[way][q]
            ring_copy(way, 1, ch).wait_recv()
            total = own[ring - 1, ch] + recv[way, 1, ch].astype(F32)
            if q < half:
                own[ring - 1, ch] = total
            else:
                out[ch] = total.T.astype(BF16)

    @pl.loop(1, middle + 1)
    def _(hops):
        for way in (RIGHT, LEFT):
            for ch in range(per):

                @pl.when(reach(way, ch) >= hops)
                def _():
                    ring_copy(way, hops, ch).wait_send()

    @pl.when(block < blocks - 1)
    def _():
        @pl.loop(0, ring)
        def _(slot):
            for part in (0, 1):
                rim_copy(slot, part).wait_send()


def body(ring, blocks, voltages, delays, tap_sets, tap_table, weights):
    _, channels, parts, antennas, time = voltages.shape
    beams = weights.shape[-1]
    per = channels // ring
    rows = parts * antennas
    hops = ring // 2 + 1
    set_count = tap_table.shape[0]
    out = pl.pallas_call(
        functools.partial(kernel, ring, blocks),
        out_shape=jax.ShapeDtypeStruct((per, 2 * beams, time), BF16),
        in_specs=[
            pl.BlockSpec(memory_space=pltpu.HBM),
            pl.BlockSpec(memory_space=pltpu.HBM),
            pl.BlockSpec(memory_space=pltpu.HBM),
            pl.BlockSpec(memory_space=pltpu.SMEM),
            pl.BlockSpec(memory_space=pltpu.HBM),
        ],
        out_specs=pl.BlockSpec(memory_space=pltpu.VMEM),
        scratch_shapes=[
            pltpu.SMEM(tap_sets.shape, jnp.int32),
            pltpu.VMEM(tap_table.shape, BF16),
            pltpu.VMEM((ring, per, rows, time), BF16),
            pltpu.VMEM((ring, per, rows, beams), BF16),
            pltpu.VMEM((ring, per, RIM, rows), BF16),
            pltpu.VMEM((ring, per, RIM, rows), BF16),
            pltpu.VMEM((set_count, time, time), BF16),
            pltpu.VMEM((set_count, RIM, RIM), BF16),
            pltpu.VMEM((2 * per, RIM, rows), F32),
            pltpu.VMEM((ring, per, time, 2 * beams), F32),
            pltpu.VMEM((2, hops, per, time, 2 * beams), BF16),
            pltpu.VMEM((2, hops, per, time, 2 * beams), BF16),
            pltpu.SemaphoreType.DMA((2,)),
            pltpu.SemaphoreType.DMA((ring, 2)),
            pltpu.SemaphoreType.DMA((ring, 2)),
            pltpu.SemaphoreType.DMA((ring, 2)),
            pltpu.SemaphoreType.DMA((2, hops, per)),
            pltpu.SemaphoreType.DMA((2, hops, per)),
        ],
        compiler_params=pltpu.CompilerParams(
            collective_id=0, has_side_effects=True, vmem_limit_bytes=63 * 1024 * 1024
        ),
    )(
        voltages.reshape(channels, rows, time),
        weights.reshape(channels, rows, beams),
        tap_sets,
        delays,
        tap_table,
    )
    return out.reshape(per, 2, beams, time)


def solution(mesh):
    return jax.shard_map(
        functools.partial(body, mesh.shape["station"], mesh.shape["tm"]),
        mesh=mesh,
        in_specs=(
            P(("group", "station"), "chan", None, None, "tm"),
            P(("group", "station")),
            P(("group", "station"), "chan"),
            P(),
            P(("group", "station"), "chan", None, None, None),
        ),
        out_specs=P(("group", "chan", "station"), None, None, "tm"),
        check_vma=False,
    )
```

```python
import functools

import jax
import jax.numpy as jnp
from jax import lax
from jax.experimental import pallas as pl
from jax.experimental.pallas import tpu as pltpu
from jax.sharding import PartitionSpec as P

TAPS = 16
MAXD = 16
RIM = 32
MESH = pl.DeviceIdType.MESH
F32 = jnp.float32
BF16 = jnp.bfloat16


RIGHT, LEFT = 0, 1


def dot_nt(left, right):
    return lax.dot_general(left, right, (((1,), (1,)), ((), ())), preferred_element_type=F32)


def kernel(
    ring,
    blocks,
    volt,
    steer,
    sets_hbm,
    delays,
    taps_hbm,
    out,
    sets,
    taps,
    vbuf,
    wbuf,
    rim_out,
    rim_in,
    band,
    band_rim,
    top,
    own,
    send,
    recv,
    small_sem,
    load_sem,
    rim_send,
    rim_recv,
    ring_send,
    ring_recv,
):
    me = lax.axis_index("station")
    block = lax.axis_index("tm")
    per = vbuf.shape[1]
    time = vbuf.shape[3]
    rows = vbuf.shape[2]
    antennas = rows // 2
    set_count = taps.shape[0]
    middle, half = ring // 2, per // 2
    sides = (lax.rem(me + 1, ring), lax.rem(me + ring - 1, ring))

    barrier = pltpu.get_barrier_semaphore()
    for side in sides:
        pl.semaphore_signal(barrier, inc=1, device_id={"station": side}, device_id_type=MESH)

    @pl.when(block > 0)
    def _():
        pl.semaphore_signal(barrier, inc=1, device_id={"tm": block - 1}, device_id_type=MESH)

    @pl.when(block < blocks - 1)
    def _():
        pl.semaphore_signal(barrier, inc=1, device_id={"tm": block + 1}, device_id_type=MESH)

    def reach(way, ch):
        right = middle - ch // half
        return right if way == RIGHT else ring - 1 - right

    def slot_of(way, hops):
        nearer = middle - hops
        near = 2 * nearer - 1 if way == RIGHT else 2 * nearer
        return max(near, 0) if isinstance(hops, int) else jnp.maximum(near, 0)

    def block_of(slot):
        odd = slot % 2
        distance = jnp.where(odd == 1, ring - (slot + 1) // 2, slot // 2)
        return lax.rem(me + middle + distance, ring)

    def load(slot, which):
        source, target = ((volt, vbuf), (steer, wbuf))[which]
        at = block_of(slot) * per
        return pltpu.make_async_copy(source.at[pl.ds(at, per)], target.at[slot], load_sem.at[slot, which])

    def start_loads(slot):
        load(slot, 0).start()
        load(slot, 1).start()

    small = [
        pltpu.make_async_copy(source, target, small_sem.at[index])
        for index, (source, target) in enumerate(((taps_hbm, taps), (sets_hbm, sets)))
    ]
    for copy in small:
        copy.start()
    start_loads(0)
    for copy in small:
        copy.wait()
    for slot in (1, 2):
        start_loads(slot)

    delay = delays[0]
    table = taps[...].astype(F32)
    lane = lax.broadcasted_iota(jnp.int32, (set_count, time), 1)
    base = jnp.zeros((set_count, time), F32)
    for tap in range(TAPS):
        base = jnp.where((lane + (tap + delay)) % time == 0, table[:, tap : tap + 1], base)
    row_at = lax.broadcasted_iota(jnp.int32, (time, time), 0)
    col_at = lax.broadcasted_iota(jnp.int32, (time, time), 1)
    for index in range(set_count):
        spread = jnp.broadcast_to(base[index : index + 1], (time, time))
        turned = pltpu.roll(spread, 0, 1, stride=1, stride_axis=0)
        band[index] = jnp.where(col_at <= row_at, turned, 0.0).astype(BF16)
        turned = pltpu.roll(spread[:RIM], RIM, 1, stride=1, stride_axis=0)
        band_rim[index] = turned[:, :RIM].astype(BF16)

    pick_row = lax.broadcasted_iota(jnp.int32, (RIM, time), 0)
    pick_col = lax.broadcasted_iota(jnp.int32, (RIM, time), 1)
    pick = jnp.where(pick_col == pick_row + (time - RIM), 1.0, 0.0).astype(BF16)

    def rim_copy(slot, part):
        pair = pl.ds(part * half, half)
        return pltpu.make_async_remote_copy(
            src_ref=rim_out.at[slot, pair],
            dst_ref=rim_in.at[slot, pair],
            send_sem=rim_send.at[slot, part],
            recv_sem=rim_recv.at[slot, part],
            device_id={"tm": lax.rem(block + 1, blocks)},
            device_id_type=MESH,
        )

    def send_rim(slot, part):
        @pl.when(block < blocks - 1)
        def _():
            for ch in range(part * half, (part + 1) * half):
                rim_out[slot, ch] = dot_nt(pick, vbuf[slot, ch]).astype(BF16)
            rim_copy(slot, part).start()

    def wait_rim(slot, part):
        @pl.when(block > 0)
        def _():
            rim_copy(slot, part).wait_recv()

    @pl.when(block == 0)
    def _():
        rim_in[...] = jnp.zeros_like(rim_in)

    def steering(slot, ch):
        real_w = wbuf[slot, ch, :antennas]
        imag_w = wbuf[slot, ch, antennas:]
        upper = jnp.concatenate([real_w, imag_w], axis=1)
        lower = jnp.concatenate([-imag_w, real_w], axis=1)
        return jnp.concatenate([upper, lower], axis=0)

    def filtered(slot, ch):
        chosen = sets[0, block_of(slot) * per + ch]
        return chosen, dot_nt(band[chosen], vbuf[slot, ch])

    def with_rim(slot, ch, chosen, early):
        return early + jnp.dot(band_rim[chosen], rim_in[slot, ch], preferred_element_type=F32)

    def beams(slot, ch):
        chosen, full = filtered(slot, ch)
        early = with_rim(slot, ch, chosen, full[:RIM])
        delayed = jnp.concatenate([early, full[RIM:]], axis=0).astype(BF16)
        return jnp.dot(delayed, steering(slot, ch), preferred_element_type=F32)

    def ring_copy(way, hops, ch, part=None):
        span = pl.ds(0, time) if part is None else part
        return pltpu.make_async_remote_copy(
            src_ref=send.at[way, hops, ch, span],
            dst_ref=recv.at[way, hops, ch, span],
            send_sem=ring_send.at[way, hops, ch],
            recv_sem=ring_recv.at[way, hops, ch],
            device_id={"station": sides[way]},
            device_id_type=MESH,
        )

    firsts = []
    for back in (0, 1):
        for q in range(half):
            firsts.append((RIGHT, middle - back, back * half + q))
            firsts.append((LEFT, middle - back, (1 - back) * half + q))
    early_span, late_span = pl.ds(0, RIM), pl.ds(RIM, time - RIM)

    def late_part(index):
        way, hops, ch = firsts[index]
        slot = slot_of(way, hops)
        chosen, full = filtered(slot, ch)
        top[index] = full[:RIM]
        late = jnp.dot(full[RIM:].astype(BF16), steering(slot, ch), preferred_element_type=F32)
        send[way, hops, ch, RIM:] = late.astype(BF16)

    def early_part(index):
        way, hops, ch = firsts[index]
        slot = slot_of(way, hops)
        chosen = sets[0, block_of(slot) * per + ch]
        early = with_rim(slot, ch, chosen, top[index]).astype(BF16)
        early = jnp.dot(early, steering(slot, ch), preferred_element_type=F32)
        send[way, hops, ch, :RIM] = early.astype(BF16)

    def leave(index, span):
        way, hops, ch = firsts[index]
        ring_copy(way, hops, ch, span).start()

    load(0, 0).wait()
    greeters = 2 + jnp.where(block > 0, 1, 0) + jnp.where(block < blocks - 1, 1, 0)
    pl.semaphore_wait(barrier, greeters)
    for part in (0, 1):
        send_rim(0, part)
    load(0, 1).wait()
    for index in range(2 * half):
        late_part(index)
        leave(index, late_span)
    for slot in (1, 2):
        load(slot, 0).wait()
        send_rim(slot, 2 - slot)
    for slot in range(3, ring):
        start_loads(slot)
    for slot in (1, 2):
        load(slot, 1).wait()
    for index in range(2 * half, 4 * half):
        late_part(index)
    for part in (0, 1):
        wait_rim(0, part)
    for index in range(2 * half):
        early_part(index)
        leave(index, early_span)
    for index in range(2 * half, 4 * half):
        leave(index, late_span)
    for slot in (1, 2):
        send_rim(slot, slot - 1)
    for slot in (1, 2):
        wait_rim(slot, 2 - slot)
    for index in range(2 * half, 4 * half):
        early_part(index)
        leave(index, early_span)

    def prepare(slot):
        load(slot, 0).wait()
        for part in (0, 1):
            send_rim(slot, part)

    def fill(slots):
        for slot in slots:
            load(slot, 1).wait()
            for part in (0, 1):
                wait_rim(slot, part)

    prepare(3)
    prepare(4)
    for slot in (1, 2):
        wait_rim(slot, slot - 1)
    for ch in range(half):
        own[1, ch] = beams(1, ch)
        own[2, ch + half] = beams(2, ch + half)
    prepare(5)
    prepare(6)

    order = ([(q + half) % per for q in range(per)], list(range(per)))

    def pass_on(way, hops, ch):
        slot = slot_of(way, hops)

        @pl.when(reach(way, ch) > hops)
        def _():
            ring_copy(way, hops + 1, ch).wait_recv()
            total = own[slot, ch] + recv[way, hops + 1, ch].astype(F32)
            send[way, hops, ch] = total.astype(BF16)
            ring_copy(way, hops, ch).start()

    @pl.loop(1, middle)
    def _(step):
        hops = middle - step
        coming = hops - 1
        slots = [slot_of(way, jnp.maximum(coming, 1)) for way in (RIGHT, LEFT)]

        for q in range(per):
            pass_on(LEFT, hops, order[LEFT][q])
            pass_on(RIGHT, hops, order[RIGHT][q])

        @pl.when(coming >= 1)
        def _():
            fill(slots)
            for q in range(per):
                for way in (RIGHT, LEFT):
                    ch = order[way][q]
                    own[slots[way], ch] = beams(slots[way], ch)

        @pl.when(coming == 0)
        def _():
            fill((ring - 1,))
            for q in range(per):
                own[ring - 1, q] = beams(ring - 1, q)

        @pl.when(coming >= 3)
        def _():
            for way in (RIGHT, LEFT):
                prepare(slot_of(way, jnp.maximum(coming - 2, 1)))

        @pl.when(coming == 2)
        def _():
            prepare(ring - 1)

    for q in range(per):
        for way in (RIGHT, LEFT):
            ch = order[way][q]
            ring_copy(way, 1, ch).wait_recv()
            total = own[ring - 1, ch] + recv[way, 1, ch].astype(F32)
            if q < half:
                own[ring - 1, ch] = total
            else:
                out[ch] = total.T.astype(BF16)

    @pl.loop(1, middle + 1)
    def _(hops):
        for way in (RIGHT, LEFT):
            for ch in range(per):

                @pl.when(reach(way, ch) >= hops)
                def _():
                    ring_copy(way, hops, ch).wait_send()

    @pl.when(block < blocks - 1)
    def _():
        @pl.loop(0, ring)
        def _(slot):
            for part in (0, 1):
                rim_copy(slot, part).wait_send()


def body(ring, blocks, voltages, delays, tap_sets, tap_table, weights):
    _, channels, parts, antennas, time = voltages.shape
    beams = weights.shape[-1]
    per = channels // ring
    rows = parts * antennas
    hops = ring // 2 + 1
    set_count = tap_table.shape[0]
    out = pl.pallas_call(
        functools.partial(kernel, ring, blocks),
        out_shape=jax.ShapeDtypeStruct((per, 2 * beams, time), BF16),
        in_specs=[
            pl.BlockSpec(memory_space=pltpu.HBM),
            pl.BlockSpec(memory_space=pltpu.HBM),
            pl.BlockSpec(memory_space=pltpu.HBM),
            pl.BlockSpec(memory_space=pltpu.SMEM),
            pl.BlockSpec(memory_space=pltpu.HBM),
        ],
        out_specs=pl.BlockSpec(memory_space=pltpu.VMEM),
        scratch_shapes=[
            pltpu.SMEM(tap_sets.shape, jnp.int32),
            pltpu.VMEM(tap_table.shape, BF16),
            pltpu.VMEM((ring, per, rows, time), BF16),
            pltpu.VMEM((ring, per, rows, beams), BF16),
            pltpu.VMEM((ring, per, RIM, rows), BF16),
            pltpu.VMEM((ring, per, RIM, rows), BF16),
            pltpu.VMEM((set_count, time, time), BF16),
            pltpu.VMEM((set_count, RIM, RIM), BF16),
            pltpu.VMEM((2 * per, RIM, rows), F32),
            pltpu.VMEM((ring, per, time, 2 * beams), F32),
            pltpu.VMEM((2, hops, per, time, 2 * beams), BF16),
            pltpu.VMEM((2, hops, per, time, 2 * beams), BF16),
            pltpu.SemaphoreType.DMA((2,)),
            pltpu.SemaphoreType.DMA((ring, 2)),
            pltpu.SemaphoreType.DMA((ring, 2)),
            pltpu.SemaphoreType.DMA((ring, 2)),
            pltpu.SemaphoreType.DMA((2, hops, per)),
            pltpu.SemaphoreType.DMA((2, hops, per)),
        ],
        compiler_params=pltpu.CompilerParams(
            collective_id=0, has_side_effects=True, vmem_limit_bytes=63 * 1024 * 1024
        ),
    )(
        voltages.reshape(channels, rows, time),
        weights.reshape(channels, rows, beams),
        tap_sets,
        delays,
        tap_table,
    )
    return out.reshape(per, 2, beams, time)


def solution(mesh):
    return jax.shard_map(
        functools.partial(body, mesh.shape["station"], mesh.shape["tm"]),
        mesh=mesh,
        in_specs=(
            P(("group", "station"), "chan", None, None, "tm"),
            P(("group", "station")),
            P(("group", "station"), "chan"),
            P(),
            P(("group", "station"), "chan", None, None, None),
        ),
        out_specs=P(("group", "chan", "station"), None, None, "tm"),
        check_vma=False,
    )
```

```python
import functools

import jax
import jax.numpy as jnp
from jax import lax
from jax.experimental import pallas as pl
from jax.experimental.pallas import tpu as pltpu
from jax.sharding import PartitionSpec as P

TAPS = 16
MAXD = 16
RIM = 32
MESH = pl.DeviceIdType.MESH
F32 = jnp.float32
BF16 = jnp.bfloat16


RIGHT, LEFT = 0, 1


def dot_nt(left, right):
    return lax.dot_general(left, right, (((1,), (1,)), ((), ())), preferred_element_type=F32)


def kernel(
    ring,
    blocks,
    volt,
    steer,
    sets_hbm,
    delays,
    taps_hbm,
    out,
    sets,
    taps,
    vbuf,
    wbuf,
    rim_out,
    rim_in,
    band,
    band_rim,
    top,
    own,
    send,
    recv,
    small_sem,
    load_sem,
    rim_send,
    rim_recv,
    ring_send,
    ring_recv,
):
    me = lax.axis_index("station")
    block = lax.axis_index("tm")
    per = vbuf.shape[1]
    time = vbuf.shape[3]
    rows = vbuf.shape[2]
    antennas = rows // 2
    set_count = taps.shape[0]
    middle, half = ring // 2, per // 2
    sides = (lax.rem(me + 1, ring), lax.rem(me + ring - 1, ring))

    barrier = pltpu.get_barrier_semaphore()
    for side in sides:
        pl.semaphore_signal(barrier, inc=1, device_id={"station": side}, device_id_type=MESH)

    @pl.when(block > 0)
    def _():
        pl.semaphore_signal(barrier, inc=1, device_id={"tm": block - 1}, device_id_type=MESH)

    @pl.when(block < blocks - 1)
    def _():
        pl.semaphore_signal(barrier, inc=1, device_id={"tm": block + 1}, device_id_type=MESH)

    def reach(way, ch):
        right = middle - ch // half
        return right if way == RIGHT else ring - 1 - right

    def slot_of(way, hops):
        nearer = middle - hops
        near = 2 * nearer - 1 if way == RIGHT else 2 * nearer
        return max(near, 0) if isinstance(hops, int) else jnp.maximum(near, 0)

    def block_of(slot):
        odd = slot % 2
        distance = jnp.where(odd == 1, ring - (slot + 1) // 2, slot // 2)
        return lax.rem(me + middle + distance, ring)

    def load(slot, which):
        source, target = ((volt, vbuf), (steer, wbuf))[which]
        at = block_of(slot) * per
        return pltpu.make_async_copy(source.at[pl.ds(at, per)], target.at[slot], load_sem.at[slot, which])

    def start_loads(slot):
        load(slot, 0).start()
        load(slot, 1).start()

    small = [
        pltpu.make_async_copy(source, target, small_sem.at[index])
        for index, (source, target) in enumerate(((taps_hbm, taps), (sets_hbm, sets)))
    ]
    for copy in small:
        copy.start()
    for slot in range(3):
        start_loads(slot)
    for copy in small:
        copy.wait()

    delay = delays[0]
    table = taps[...].astype(F32)
    lane = lax.broadcasted_iota(jnp.int32, (set_count, time), 1)
    base = jnp.zeros((set_count, time), F32)
    for tap in range(TAPS):
        base = jnp.where((lane + (tap + delay)) % time == 0, table[:, tap : tap + 1], base)
    row_at = lax.broadcasted_iota(jnp.int32, (time, time), 0)
    col_at = lax.broadcasted_iota(jnp.int32, (time, time), 1)
    for index in range(set_count):
        spread = jnp.broadcast_to(base[index : index + 1], (time, time))
        turned = pltpu.roll(spread, 0, 1, stride=1, stride_axis=0)
        band[index] = jnp.where(col_at <= row_at, turned, 0.0).astype(BF16)
        turned = pltpu.roll(spread[:RIM], RIM, 1, stride=1, stride_axis=0)
        band_rim[index] = turned[:, :RIM].astype(BF16)

    pick_row = lax.broadcasted_iota(jnp.int32, (RIM, time), 0)
    pick_col = lax.broadcasted_iota(jnp.int32, (RIM, time), 1)
    pick = jnp.where(pick_col == pick_row + (time - RIM), 1.0, 0.0).astype(BF16)

    def rim_copy(slot, part):
        pair = pl.ds(part * half, half)
        return pltpu.make_async_remote_copy(
            src_ref=rim_out.at[slot, pair],
            dst_ref=rim_in.at[slot, pair],
            send_sem=rim_send.at[slot, part],
            recv_sem=rim_recv.at[slot, part],
            device_id={"tm": lax.rem(block + 1, blocks)},
            device_id_type=MESH,
        )

    def send_rim(slot, part):
        @pl.when(block < blocks - 1)
        def _():
            for ch in range(part * half, (part + 1) * half):
                rim_out[slot, ch] = dot_nt(pick, vbuf[slot, ch]).astype(BF16)
            rim_copy(slot, part).start()

    def wait_rim(slot, part):
        @pl.when(block > 0)
        def _():
            rim_copy(slot, part).wait_recv()

    @pl.when(block == 0)
    def _():
        rim_in[...] = jnp.zeros_like(rim_in)

    def steering(slot, ch):
        real_w = wbuf[slot, ch, :antennas]
        imag_w = wbuf[slot, ch, antennas:]
        upper = jnp.concatenate([real_w, imag_w], axis=1)
        lower = jnp.concatenate([-imag_w, real_w], axis=1)
        return jnp.concatenate([upper, lower], axis=0)

    def filtered(slot, ch):
        chosen = sets[0, block_of(slot) * per + ch]
        return chosen, dot_nt(band[chosen], vbuf[slot, ch])

    def with_rim(slot, ch, chosen, early):
        return early + jnp.dot(band_rim[chosen], rim_in[slot, ch], preferred_element_type=F32)

    def beams(slot, ch):
        chosen, full = filtered(slot, ch)
        early = with_rim(slot, ch, chosen, full[:RIM])
        delayed = jnp.concatenate([early, full[RIM:]], axis=0).astype(BF16)
        return jnp.dot(delayed, steering(slot, ch), preferred_element_type=F32)

    def ring_copy(way, hops, ch, part=None):
        span = pl.ds(0, time) if part is None else part
        return pltpu.make_async_remote_copy(
            src_ref=send.at[way, hops, ch, span],
            dst_ref=recv.at[way, hops, ch, span],
            send_sem=ring_send.at[way, hops, ch],
            recv_sem=ring_recv.at[way, hops, ch],
            device_id={"station": sides[way]},
            device_id_type=MESH,
        )

    firsts = []
    for back in (0, 1):
        for q in range(half):
            firsts.append((RIGHT, middle - back, back * half + q))
            firsts.append((LEFT, middle - back, (1 - back) * half + q))
    early_span, late_span = pl.ds(0, RIM), pl.ds(RIM, time - RIM)

    def late_part(index):
        way, hops, ch = firsts[index]
        slot = slot_of(way, hops)
        chosen, full = filtered(slot, ch)
        top[index] = full[:RIM]
        late = jnp.dot(full[RIM:].astype(BF16), steering(slot, ch), preferred_element_type=F32)
        send[way, hops, ch, RIM:] = late.astype(BF16)

    def early_part(index):
        way, hops, ch = firsts[index]
        slot = slot_of(way, hops)
        chosen = sets[0, block_of(slot) * per + ch]
        early = with_rim(slot, ch, chosen, top[index]).astype(BF16)
        early = jnp.dot(early, steering(slot, ch), preferred_element_type=F32)
        send[way, hops, ch, :RIM] = early.astype(BF16)

    def leave(index, span):
        way, hops, ch = firsts[index]
        ring_copy(way, hops, ch, span).start()

    load(0, 0).wait()
    load(0, 1).wait()
    for index in range(2 * half):
        late_part(index)
    greeters = 2 + jnp.where(block > 0, 1, 0) + jnp.where(block < blocks - 1, 1, 0)
    pl.semaphore_wait(barrier, greeters)
    for index in range(2 * half):
        leave(index, late_span)
    for part in (0, 1):
        send_rim(0, part)
    for slot in (1, 2):
        load(slot, 0).wait()
        send_rim(slot, 2 - slot)
    for slot in (1, 2):
        load(slot, 1).wait()
    for index in range(2 * half, 4 * half):
        late_part(index)
        leave(index, late_span)
    for slot in range(3, ring):
        start_loads(slot)
    for slot in (1, 2):
        send_rim(slot, slot - 1)
    for part in (0, 1):
        wait_rim(0, part)
    for index in range(2 * half):
        early_part(index)
        leave(index, early_span)
    for slot in (1, 2):
        wait_rim(slot, 2 - slot)
    for index in range(2 * half, 4 * half):
        early_part(index)
        leave(index, early_span)

    def prepare(slot):
        load(slot, 0).wait()
        for part in (0, 1):
            send_rim(slot, part)

    def fill(slots):
        for slot in slots:
            load(slot, 1).wait()
            for part in (0, 1):
                wait_rim(slot, part)

    prepare(3)
    prepare(4)
    for slot in (1, 2):
        wait_rim(slot, slot - 1)
    for ch in range(half):
        own[1, ch] = beams(1, ch)
        own[2, ch + half] = beams(2, ch + half)
    prepare(5)
    prepare(6)

    order = ([(q + half) % per for q in range(per)], list(range(per)))

    def pass_on(way, hops, ch):
        slot = slot_of(way, hops)

        @pl.when(reach(way, ch) > hops)
        def _():
            ring_copy(way, hops + 1, ch).wait_recv()
            total = own[slot, ch] + recv[way, hops + 1, ch].astype(F32)
            send[way, hops, ch] = total.astype(BF16)
            ring_copy(way, hops, ch).start()

    @pl.loop(1, middle)
    def _(step):
        hops = middle - step
        coming = hops - 1
        slots = [slot_of(way, jnp.maximum(coming, 1)) for way in (RIGHT, LEFT)]

        for q in range(per):
            pass_on(LEFT, hops, order[LEFT][q])
            pass_on(RIGHT, hops, order[RIGHT][q])

        @pl.when(coming >= 1)
        def _():
            fill(slots)
            for q in range(per):
                for way in (RIGHT, LEFT):
                    ch = order[way][q]
                    own[slots[way], ch] = beams(slots[way], ch)

        @pl.when(coming == 0)
        def _():
            fill((ring - 1,))
            for q in range(per):
                own[ring - 1, q] = beams(ring - 1, q)

        @pl.when(coming >= 3)
        def _():
            for way in (RIGHT, LEFT):
                prepare(slot_of(way, jnp.maximum(coming - 2, 1)))

        @pl.when(coming == 2)
        def _():
            prepare(ring - 1)

    for q in range(per):
        for way in (RIGHT, LEFT):
            ch = order[way][q]
            ring_copy(way, 1, ch).wait_recv()
            total = own[ring - 1, ch] + recv[way, 1, ch].astype(F32)
            if q < half:
                own[ring - 1, ch] = total
            else:
                out[ch] = total.T.astype(BF16)

    @pl.loop(1, middle + 1)
    def _(hops):
        for way in (RIGHT, LEFT):
            for ch in range(per):

                @pl.when(reach(way, ch) >= hops)
                def _():
                    ring_copy(way, hops, ch).wait_send()

    @pl.when(block < blocks - 1)
    def _():
        @pl.loop(0, ring)
        def _(slot):
            for part in (0, 1):
                rim_copy(slot, part).wait_send()


def body(ring, blocks, voltages, delays, tap_sets, tap_table, weights):
    _, channels, parts, antennas, time = voltages.shape
    beams = weights.shape[-1]
    per = channels // ring
    rows = parts * antennas
    hops = ring // 2 + 1
    set_count = tap_table.shape[0]
    out = pl.pallas_call(
        functools.partial(kernel, ring, blocks),
        out_shape=jax.ShapeDtypeStruct((per, 2 * beams, time), BF16),
        in_specs=[
            pl.BlockSpec(memory_space=pltpu.HBM),
            pl.BlockSpec(memory_space=pltpu.HBM),
            pl.BlockSpec(memory_space=pltpu.HBM),
            pl.BlockSpec(memory_space=pltpu.SMEM),
            pl.BlockSpec(memory_space=pltpu.HBM),
        ],
        out_specs=pl.BlockSpec(memory_space=pltpu.VMEM),
        scratch_shapes=[
            pltpu.SMEM(tap_sets.shape, jnp.int32),
            pltpu.VMEM(tap_table.shape, BF16),
            pltpu.VMEM((ring, per, rows, time), BF16),
            pltpu.VMEM((ring, per, rows, beams), BF16),
            pltpu.VMEM((ring, per, RIM, rows), BF16),
            pltpu.VMEM((ring, per, RIM, rows), BF16),
            pltpu.VMEM((set_count, time, time), BF16),
            pltpu.VMEM((set_count, RIM, RIM), BF16),
            pltpu.VMEM((2 * per, RIM, rows), F32),
            pltpu.VMEM((ring, per, time, 2 * beams), F32),
            pltpu.VMEM((2, hops, per, time, 2 * beams), BF16),
            pltpu.VMEM((2, hops, per, time, 2 * beams), BF16),
            pltpu.SemaphoreType.DMA((2,)),
            pltpu.SemaphoreType.DMA((ring, 2)),
            pltpu.SemaphoreType.DMA((ring, 2)),
            pltpu.SemaphoreType.DMA((ring, 2)),
            pltpu.SemaphoreType.DMA((2, hops, per)),
            pltpu.SemaphoreType.DMA((2, hops, per)),
        ],
        compiler_params=pltpu.CompilerParams(
            collective_id=0, has_side_effects=True, vmem_limit_bytes=53 * 1024 * 1024
        ),
    )(
        voltages.reshape(channels, rows, time),
        weights.reshape(channels, rows, beams),
        tap_sets,
        delays,
        tap_table,
    )
    return out.reshape(per, 2, beams, time)


def solution(mesh):
    return jax.shard_map(
        functools.partial(body, mesh.shape["station"], mesh.shape["tm"]),
        mesh=mesh,
        in_specs=(
            P(("group", "station"), "chan", None, None, "tm"),
            P(("group", "station")),
            P(("group", "station"), "chan"),
            P(),
            P(("group", "station"), "chan", None, None, None),
        ),
        out_specs=P(("group", "chan", "station"), None, None, "tm"),
        check_vma=False,
    )
```

```python
import functools

import jax
import jax.numpy as jnp
from jax import lax
from jax.experimental import pallas as pl
from jax.experimental.pallas import tpu as pltpu
from jax.sharding import PartitionSpec as P

TAPS = 16
MAXD = 16
RIM = 32
MESH = pl.DeviceIdType.MESH
F32 = jnp.float32
BF16 = jnp.bfloat16


RIGHT, LEFT = 0, 1


def dot_nt(left, right):
    return lax.dot_general(left, right, (((1,), (1,)), ((), ())), preferred_element_type=F32)


def kernel(
    ring,
    blocks,
    volt,
    steer,
    sets_hbm,
    delays,
    taps_hbm,
    out,
    sets,
    taps,
    vbuf,
    wbuf,
    rim_out,
    rim_in,
    band,
    band_rim,
    top,
    own,
    send,
    recv,
    small_sem,
    load_sem,
    rim_send,
    rim_recv,
    ring_send,
    ring_recv,
):
    me = lax.axis_index("station")
    block = lax.axis_index("tm")
    core = lax.axis_index("chan")
    per = vbuf.shape[1]
    time = vbuf.shape[3]
    rows = vbuf.shape[2]
    antennas = rows // 2
    set_count = taps.shape[0]
    middle, half = ring // 2, per // 2
    sides = (lax.rem(me + 1, ring), lax.rem(me + ring - 1, ring))

    barrier = pltpu.get_barrier_semaphore()
    for side in sides:
        pl.semaphore_signal(barrier, inc=1, device_id={"station": side}, device_id_type=MESH)

    @pl.when(block > 0)
    def _():
        pl.semaphore_signal(barrier, inc=1, device_id={"tm": block - 1}, device_id_type=MESH)

    @pl.when(block < blocks - 1)
    def _():
        pl.semaphore_signal(barrier, inc=1, device_id={"tm": block + 1}, device_id_type=MESH)

    def reach(way, ch):
        right = middle - ch // half
        return right if way == RIGHT else ring - 1 - right

    def slot_of(way, hops):
        nearer = middle - hops
        near = 2 * nearer - 1 if way == RIGHT else 2 * nearer
        return max(near, 0) if isinstance(hops, int) else jnp.maximum(near, 0)

    def block_of(slot):
        odd = slot % 2
        distance = jnp.where(odd == 1, ring - (slot + 1) // 2, slot // 2)
        return lax.rem(me + middle + distance, ring)

    def load(slot, which):
        source, target = ((volt, vbuf), (steer, wbuf))[which]
        at = block_of(slot) * per
        return pltpu.make_async_copy(source.at[pl.ds(at, per)], target.at[slot], load_sem.at[slot, which])

    def start_loads(slot):
        load(slot, 0).start()
        load(slot, 1).start()

    small = [
        pltpu.make_async_copy(source, target, small_sem.at[index])
        for index, (source, target) in enumerate(((taps_hbm, taps), (sets_hbm, sets)))
    ]
    for copy in small:
        copy.start()
    for slot in range(3):
        start_loads(slot)
    for copy in small:
        copy.wait()

    delay = delays[0]
    table = taps[...].astype(F32)
    lane = lax.broadcasted_iota(jnp.int32, (set_count, time), 1)
    base = jnp.zeros((set_count, time), F32)
    for tap in range(TAPS):
        base = jnp.where((lane + (tap + delay)) % time == 0, table[:, tap : tap + 1], base)
    row_at = lax.broadcasted_iota(jnp.int32, (time, time), 0)
    col_at = lax.broadcasted_iota(jnp.int32, (time, time), 1)
    for index in range(set_count):
        spread = jnp.broadcast_to(base[index : index + 1], (time, time))
        turned = pltpu.roll(spread, 0, 1, stride=1, stride_axis=0)
        band[index] = jnp.where(col_at <= row_at, turned, 0.0).astype(BF16)
        turned = pltpu.roll(spread[:RIM], RIM, 1, stride=1, stride_axis=0)
        band_rim[index] = turned[:, :RIM].astype(BF16)

    pick_row = lax.broadcasted_iota(jnp.int32, (RIM, time), 0)
    pick_col = lax.broadcasted_iota(jnp.int32, (RIM, time), 1)
    pick = jnp.where(pick_col == pick_row + (time - RIM), 1.0, 0.0).astype(BF16)

    def rim_copy(slot, part):
        pair = pl.ds(part * half, half)
        return pltpu.make_async_remote_copy(
            src_ref=rim_out.at[slot, pair],
            dst_ref=rim_in.at[slot, pair],
            send_sem=rim_send.at[slot, part],
            recv_sem=rim_recv.at[slot, part],
            device_id={"tm": lax.rem(block + 1, blocks)},
            device_id_type=MESH,
        )

    def send_rim(slot, part):
        @pl.when(block < blocks - 1)
        def _():
            for ch in range(part * half, (part + 1) * half):
                rim_out[slot, ch] = dot_nt(pick, vbuf[slot, ch]).astype(BF16)
            rim_copy(slot, part).start()

    def wait_rim(slot, part):
        @pl.when(block > 0)
        def _():
            rim_copy(slot, part).wait_recv()

    @pl.when(block == 0)
    def _():
        rim_in[...] = jnp.zeros_like(rim_in)

    def steering(slot, ch):
        real_w = wbuf[slot, ch, :antennas]
        imag_w = wbuf[slot, ch, antennas:]
        upper = jnp.concatenate([real_w, imag_w], axis=1)
        lower = jnp.concatenate([-imag_w, real_w], axis=1)
        return jnp.concatenate([upper, lower], axis=0)

    def filtered(slot, ch):
        chosen = sets[0, block_of(slot) * per + ch]
        return chosen, dot_nt(band[chosen], vbuf[slot, ch])

    def with_rim(slot, ch, chosen, early):
        return early + jnp.dot(band_rim[chosen], rim_in[slot, ch], preferred_element_type=F32)

    def beams(slot, ch):
        chosen, full = filtered(slot, ch)
        early = with_rim(slot, ch, chosen, full[:RIM])
        delayed = jnp.concatenate([early, full[RIM:]], axis=0).astype(BF16)
        return jnp.dot(delayed, steering(slot, ch), preferred_element_type=F32)

    def ring_copy(way, hops, ch, part=None):
        span = pl.ds(0, time) if part is None else part
        return pltpu.make_async_remote_copy(
            src_ref=send.at[way, hops, ch, span],
            dst_ref=recv.at[way, hops, ch, span],
            send_sem=ring_send.at[way, hops, ch],
            recv_sem=ring_recv.at[way, hops, ch],
            device_id={"station": sides[way]},
            device_id_type=MESH,
        )

    firsts = []
    for back in (0, 1):
        for q in range(half):
            firsts.append((RIGHT, middle - back, back * half + q))
            firsts.append((LEFT, middle - back, (1 - back) * half + q))
    early_span, late_span = pl.ds(0, RIM), pl.ds(RIM, time - RIM)

    def late_part(index):
        way, hops, ch = firsts[index]
        slot = slot_of(way, hops)
        chosen, full = filtered(slot, ch)
        top[index] = full[:RIM]
        late = jnp.dot(full[RIM:].astype(BF16), steering(slot, ch), preferred_element_type=F32)
        send[way, hops, ch, RIM:] = late.astype(BF16)

    def early_part(index):
        way, hops, ch = firsts[index]
        slot = slot_of(way, hops)
        chosen = sets[0, block_of(slot) * per + ch]
        early = with_rim(slot, ch, chosen, top[index]).astype(BF16)
        early = jnp.dot(early, steering(slot, ch), preferred_element_type=F32)
        send[way, hops, ch, :RIM] = early.astype(BF16)

    def leave(index, span):
        way, hops, ch = firsts[index]
        ring_copy(way, hops, ch, span).start()

    load(0, 0).wait()
    load(0, 1).wait()
    for index in range(2 * half):
        late_part(index)
    greeters = 2 + jnp.where(block > 0, 1, 0) + jnp.where(block < blocks - 1, 1, 0)
    pl.semaphore_wait(barrier, greeters)
    for index in range(2 * half):
        leave(index, late_span)
    for part in (0, 1):
        send_rim(0, part)
    for slot in (1, 2):
        load(slot, 0).wait()
        send_rim(slot, 2 - slot)
    for slot in (1, 2):
        load(slot, 1).wait()
    for index in range(2 * half, 4 * half):
        late_part(index)
        leave(index, late_span)
    for slot in range(3, ring):
        start_loads(slot)
    for slot in (1, 2):
        send_rim(slot, slot - 1)
    for part in (0, 1):
        wait_rim(0, part)
    for index in range(2 * half):
        early_part(index)
        leave(index, early_span)
    for slot in (1, 2):
        wait_rim(slot, 2 - slot)
    for index in range(2 * half, 4 * half):
        early_part(index)
        leave(index, early_span)

    def prepare(slot):
        load(slot, 0).wait()
        for part in (0, 1):
            send_rim(slot, part)

    def fill(slots):
        for slot in slots:
            load(slot, 1).wait()
            for part in (0, 1):
                wait_rim(slot, part)

    prepare(3)
    prepare(4)
    for slot in (1, 2):
        wait_rim(slot, slot - 1)
    for ch in range(half):
        own[1, ch] = beams(1, ch)
        own[2, ch + half] = beams(2, ch + half)
    prepare(5)
    prepare(6)

    order = ([(q + half) % per for q in range(per)], list(range(per)))

    def pass_on(way, hops, ch, now):
        slot = slot_of(way, hops)

        @pl.when(jnp.logical_and(reach(way, ch) > hops, now))
        def _():
            ring_copy(way, hops + 1, ch).wait_recv()
            total = own[slot, ch] + recv[way, hops + 1, ch].astype(F32)
            send[way, hops, ch] = total.astype(BF16)
            ring_copy(way, hops, ch).start()

    @pl.loop(1, middle)
    def _(step):
        hops = middle - step
        coming = hops - 1
        slots = [slot_of(way, jnp.maximum(coming, 1)) for way in (RIGHT, LEFT)]

        for q in range(per):
            pass_on(LEFT, hops, order[LEFT][q], core == 0)
            pass_on(RIGHT, hops, order[RIGHT][q], True)
            pass_on(LEFT, hops, order[LEFT][q], core == 1)

        @pl.when(coming >= 1)
        def _():
            fill(slots)
            for q in range(per):
                for way in (RIGHT, LEFT):
                    ch = order[way][q]
                    own[slots[way], ch] = beams(slots[way], ch)

        @pl.when(coming == 0)
        def _():
            fill((ring - 1,))
            for q in range(per):
                own[ring - 1, q] = beams(ring - 1, q)

        @pl.when(coming >= 3)
        def _():
            for way in (RIGHT, LEFT):
                prepare(slot_of(way, jnp.maximum(coming - 2, 1)))

        @pl.when(coming == 2)
        def _():
            prepare(ring - 1)

    for q in range(per):
        for way in (RIGHT, LEFT):
            ch = order[way][q]
            ring_copy(way, 1, ch).wait_recv()
            total = own[ring - 1, ch] + recv[way, 1, ch].astype(F32)
            if q < half:
                own[ring - 1, ch] = total
            else:
                out[ch] = total.T.astype(BF16)

    @pl.loop(1, middle + 1)
    def _(hops):
        for way in (RIGHT, LEFT):
            for ch in range(per):

                @pl.when(reach(way, ch) >= hops)
                def _():
                    ring_copy(way, hops, ch).wait_send()

    @pl.when(block < blocks - 1)
    def _():
        @pl.loop(0, ring)
        def _(slot):
            for part in (0, 1):
                rim_copy(slot, part).wait_send()


def body(ring, blocks, voltages, delays, tap_sets, tap_table, weights):
    _, channels, parts, antennas, time = voltages.shape
    beams = weights.shape[-1]
    per = channels // ring
    rows = parts * antennas
    hops = ring // 2 + 1
    set_count = tap_table.shape[0]
    out = pl.pallas_call(
        functools.partial(kernel, ring, blocks),
        out_shape=jax.ShapeDtypeStruct((per, 2 * beams, time), BF16),
        in_specs=[
            pl.BlockSpec(memory_space=pltpu.HBM),
            pl.BlockSpec(memory_space=pltpu.HBM),
            pl.BlockSpec(memory_space=pltpu.HBM),
            pl.BlockSpec(memory_space=pltpu.SMEM),
            pl.BlockSpec(memory_space=pltpu.HBM),
        ],
        out_specs=pl.BlockSpec(memory_space=pltpu.VMEM),
        scratch_shapes=[
            pltpu.SMEM(tap_sets.shape, jnp.int32),
            pltpu.VMEM(tap_table.shape, BF16),
            pltpu.VMEM((ring, per, rows, time), BF16),
            pltpu.VMEM((ring, per, rows, beams), BF16),
            pltpu.VMEM((ring, per, RIM, rows), BF16),
            pltpu.VMEM((ring, per, RIM, rows), BF16),
            pltpu.VMEM((set_count, time, time), BF16),
            pltpu.VMEM((set_count, RIM, RIM), BF16),
            pltpu.VMEM((2 * per, RIM, rows), F32),
            pltpu.VMEM((ring, per, time, 2 * beams), F32),
            pltpu.VMEM((2, hops, per, time, 2 * beams), BF16),
            pltpu.VMEM((2, hops, per, time, 2 * beams), BF16),
            pltpu.SemaphoreType.DMA((2,)),
            pltpu.SemaphoreType.DMA((ring, 2)),
            pltpu.SemaphoreType.DMA((ring, 2)),
            pltpu.SemaphoreType.DMA((ring, 2)),
            pltpu.SemaphoreType.DMA((2, hops, per)),
            pltpu.SemaphoreType.DMA((2, hops, per)),
        ],
        compiler_params=pltpu.CompilerParams(
            collective_id=0, has_side_effects=True, vmem_limit_bytes=53 * 1024 * 1024
        ),
    )(
        voltages.reshape(channels, rows, time),
        weights.reshape(channels, rows, beams),
        tap_sets,
        delays,
        tap_table,
    )
    return out.reshape(per, 2, beams, time)


def solution(mesh):
    return jax.shard_map(
        functools.partial(body, mesh.shape["station"], mesh.shape["tm"]),
        mesh=mesh,
        in_specs=(
            P(("group", "station"), "chan", None, None, "tm"),
            P(("group", "station")),
            P(("group", "station"), "chan"),
            P(),
            P(("group", "station"), "chan", None, None, None),
        ),
        out_specs=P(("group", "chan", "station"), None, None, "tm"),
        check_vma=False,
    )
```

```python
import functools

import jax
import jax.numpy as jnp
from jax import lax
from jax.experimental import pallas as pl
from jax.experimental.pallas import tpu as pltpu
from jax.sharding import PartitionSpec as P

TAPS = 16
MAXD = 16
RIM = 32
MESH = pl.DeviceIdType.MESH
F32 = jnp.float32
BF16 = jnp.bfloat16


RIGHT, LEFT = 0, 1


def dot_nt(left, right):
    return lax.dot_general(left, right, (((1,), (1,)), ((), ())), preferred_element_type=F32)


def kernel(
    ring,
    blocks,
    volt,
    steer,
    sets_hbm,
    delays,
    taps_hbm,
    out,
    sets,
    taps,
    vbuf,
    wbuf,
    rim_out,
    rim_in,
    band,
    band_rim,
    top,
    own,
    send,
    recv,
    small_sem,
    load_sem,
    rim_send,
    rim_recv,
    ring_send,
    ring_recv,
):
    me = lax.axis_index("station")
    block = lax.axis_index("tm")
    per = vbuf.shape[1]
    time = vbuf.shape[3]
    rows = vbuf.shape[2]
    antennas = rows // 2
    set_count = taps.shape[0]
    middle, half = ring // 2, per // 2
    sides = (lax.rem(me + 1, ring), lax.rem(me + ring - 1, ring))

    barrier = pltpu.get_barrier_semaphore()
    for side in sides:
        pl.semaphore_signal(barrier, inc=1, device_id={"station": side}, device_id_type=MESH)

    @pl.when(block > 0)
    def _():
        pl.semaphore_signal(barrier, inc=1, device_id={"tm": block - 1}, device_id_type=MESH)

    @pl.when(block < blocks - 1)
    def _():
        pl.semaphore_signal(barrier, inc=1, device_id={"tm": block + 1}, device_id_type=MESH)

    def reach(way, ch):
        right = middle - ch // half
        return right if way == RIGHT else ring - 1 - right

    def slot_of(way, hops):
        nearer = middle - hops
        near = 2 * nearer - 1 if way == RIGHT else 2 * nearer
        return max(near, 0) if isinstance(hops, int) else jnp.maximum(near, 0)

    def block_of(slot):
        odd = slot % 2
        distance = jnp.where(odd == 1, ring - (slot + 1) // 2, slot // 2)
        return lax.rem(me + middle + distance, ring)

    def load(slot, which):
        source, target = ((volt, vbuf), (steer, wbuf))[which]
        at = block_of(slot) * per
        return pltpu.make_async_copy(source.at[pl.ds(at, per)], target.at[slot], load_sem.at[slot, which])

    def start_loads(slot):
        load(slot, 0).start()
        load(slot, 1).start()

    small = [
        pltpu.make_async_copy(source, target, small_sem.at[index])
        for index, (source, target) in enumerate(((taps_hbm, taps), (sets_hbm, sets)))
    ]
    for copy in small:
        copy.start()
    for slot in range(3):
        start_loads(slot)
    for copy in small:
        copy.wait()

    delay = delays[0]
    table = taps[...].astype(F32)
    lane = lax.broadcasted_iota(jnp.int32, (set_count, time), 1)
    base = jnp.zeros((set_count, time), F32)
    for tap in range(TAPS):
        base = jnp.where((lane + (tap + delay)) % time == 0, table[:, tap : tap + 1], base)
    row_at = lax.broadcasted_iota(jnp.int32, (time, time), 0)
    col_at = lax.broadcasted_iota(jnp.int32, (time, time), 1)
    for index in range(set_count):
        spread = jnp.broadcast_to(base[index : index + 1], (time, time))
        turned = pltpu.roll(spread, 0, 1, stride=1, stride_axis=0)
        band[index] = jnp.where(col_at <= row_at, turned, 0.0).astype(BF16)
        turned = pltpu.roll(spread[:RIM], RIM, 1, stride=1, stride_axis=0)
        band_rim[index] = turned[:, :RIM].astype(BF16)

    pick_row = lax.broadcasted_iota(jnp.int32, (RIM, time), 0)
    pick_col = lax.broadcasted_iota(jnp.int32, (RIM, time), 1)
    pick = jnp.where(pick_col == pick_row + (time - RIM), 1.0, 0.0).astype(BF16)

    def rim_copy(slot, part):
        pair = pl.ds(part * half, half)
        return pltpu.make_async_remote_copy(
            src_ref=rim_out.at[slot, pair],
            dst_ref=rim_in.at[slot, pair],
            send_sem=rim_send.at[slot, part],
            recv_sem=rim_recv.at[slot, part],
            device_id={"tm": lax.rem(block + 1, blocks)},
            device_id_type=MESH,
        )

    def send_rim(slot, part):
        @pl.when(block < blocks - 1)
        def _():
            for ch in range(part * half, (part + 1) * half):
                rim_out[slot, ch] = dot_nt(pick, vbuf[slot, ch]).astype(BF16)
            rim_copy(slot, part).start()

    def wait_rim(slot, part):
        @pl.when(block > 0)
        def _():
            rim_copy(slot, part).wait_recv()

    @pl.when(block == 0)
    def _():
        rim_in[...] = jnp.zeros_like(rim_in)

    def steering(slot, ch):
        real_w = wbuf[slot, ch, :antennas]
        imag_w = wbuf[slot, ch, antennas:]
        upper = jnp.concatenate([real_w, imag_w], axis=1)
        lower = jnp.concatenate([-imag_w, real_w], axis=1)
        return jnp.concatenate([upper, lower], axis=0)

    def filtered(slot, ch):
        chosen = sets[0, block_of(slot) * per + ch]
        return chosen, dot_nt(band[chosen], vbuf[slot, ch])

    def with_rim(slot, ch, chosen, early):
        return early + jnp.dot(band_rim[chosen], rim_in[slot, ch], preferred_element_type=F32)

    def beams(slot, ch):
        chosen, full = filtered(slot, ch)
        early = with_rim(slot, ch, chosen, full[:RIM])
        delayed = jnp.concatenate([early, full[RIM:]], axis=0).astype(BF16)
        return jnp.dot(delayed, steering(slot, ch), preferred_element_type=F32)

    def ring_copy(way, hops, ch, part=None):
        span = pl.ds(0, time) if part is None else part
        return pltpu.make_async_remote_copy(
            src_ref=send.at[way, hops, ch, span],
            dst_ref=recv.at[way, hops, ch, span],
            send_sem=ring_send.at[way, hops, ch],
            recv_sem=ring_recv.at[way, hops, ch],
            device_id={"station": sides[way]},
            device_id_type=MESH,
        )

    firsts = []
    for back in (0, 1):
        for q in range(half):
            firsts.append((RIGHT, middle - back, back * half + q))
            firsts.append((LEFT, middle - back, (1 - back) * half + q))
    early_span, late_span = pl.ds(0, RIM), pl.ds(RIM, time - RIM)

    def late_part(index):
        way, hops, ch = firsts[index]
        slot = slot_of(way, hops)
        chosen, full = filtered(slot, ch)
        top[index] = full[:RIM]
        late = jnp.dot(full[RIM:].astype(BF16), steering(slot, ch), preferred_element_type=F32)
        send[way, hops, ch, RIM:] = late.astype(BF16)

    def early_part(index):
        way, hops, ch = firsts[index]
        slot = slot_of(way, hops)
        chosen = sets[0, block_of(slot) * per + ch]
        early = with_rim(slot, ch, chosen, top[index]).astype(BF16)
        early = jnp.dot(early, steering(slot, ch), preferred_element_type=F32)
        send[way, hops, ch, :RIM] = early.astype(BF16)

    def leave(index, span):
        way, hops, ch = firsts[index]
        ring_copy(way, hops, ch, span).start()

    load(0, 0).wait()
    load(0, 1).wait()
    for index in range(2 * half):
        late_part(index)
    greeters = 2 + jnp.where(block > 0, 1, 0) + jnp.where(block < blocks - 1, 1, 0)
    pl.semaphore_wait(barrier, greeters)
    for index in range(2 * half):
        leave(index, late_span)
    for part in (0, 1):
        send_rim(0, part)
    for slot in (1, 2):
        load(slot, 0).wait()
        send_rim(slot, 2 - slot)
    for slot in (1, 2):
        load(slot, 1).wait()
    for index in range(2 * half, 4 * half):
        late_part(index)
        leave(index, late_span)
    for slot in range(3, ring):
        start_loads(slot)
    for slot in (1, 2):
        send_rim(slot, slot - 1)
    for part in (0, 1):
        wait_rim(0, part)
    for index in range(2 * half):
        early_part(index)
        leave(index, early_span)
    for slot in (1, 2):
        wait_rim(slot, 2 - slot)
    for index in range(2 * half, 4 * half):
        early_part(index)
        leave(index, early_span)

    def prepare(slot):
        load(slot, 0).wait()
        for part in (0, 1):
            send_rim(slot, part)

    def fill(slots):
        for slot in slots:
            load(slot, 1).wait()
            for part in (0, 1):
                wait_rim(slot, part)

    prepare(3)
    prepare(4)
    for slot in (1, 2):
        wait_rim(slot, slot - 1)
    for ch in range(half):
        own[1, ch] = beams(1, ch)
        own[2, ch + half] = beams(2, ch + half)
    prepare(5)
    prepare(6)

    order = ([(q + half) % per for q in range(per)], list(range(per)))

    def pass_on(way, hops, ch):
        slot = slot_of(way, hops)

        @pl.when(reach(way, ch) > hops)
        def _():
            ring_copy(way, hops + 1, ch).wait_recv()
            total = own[slot, ch] + recv[way, hops + 1, ch].astype(F32)
            send[way, hops, ch] = total.astype(BF16)
            ring_copy(way, hops, ch).start()

    @pl.loop(1, middle)
    def _(step):
        hops = middle - step
        coming = hops - 1
        slots = [slot_of(way, jnp.maximum(coming, 1)) for way in (RIGHT, LEFT)]

        for q in range(per):
            pass_on(LEFT, hops, order[LEFT][q])
            pass_on(RIGHT, hops, order[RIGHT][q])

        @pl.when(coming >= 3)
        def _():
            for way in (RIGHT, LEFT):
                prepare(slot_of(way, jnp.maximum(coming - 2, 1)))

        @pl.when(coming == 2)
        def _():
            prepare(ring - 1)

        @pl.when(coming >= 1)
        def _():
            fill(slots)
            for q in range(per):
                for way in (RIGHT, LEFT):
                    ch = order[way][q]
                    own[slots[way], ch] = beams(slots[way], ch)

        @pl.when(coming == 0)
        def _():
            fill((ring - 1,))
            for q in range(per):
                own[ring - 1, q] = beams(ring - 1, q)

    for q in range(per):
        for way in (RIGHT, LEFT):
            ch = order[way][q]
            ring_copy(way, 1, ch).wait_recv()
            total = own[ring - 1, ch] + recv[way, 1, ch].astype(F32)
            if q < half:
                own[ring - 1, ch] = total
            else:
                out[ch] = total.T.astype(BF16)

    @pl.loop(1, middle + 1)
    def _(hops):
        for way in (RIGHT, LEFT):
            for ch in range(per):

                @pl.when(reach(way, ch) >= hops)
                def _():
                    ring_copy(way, hops, ch).wait_send()

    @pl.when(block < blocks - 1)
    def _():
        @pl.loop(0, ring)
        def _(slot):
            for part in (0, 1):
                rim_copy(slot, part).wait_send()


def body(ring, blocks, voltages, delays, tap_sets, tap_table, weights):
    _, channels, parts, antennas, time = voltages.shape
    beams = weights.shape[-1]
    per = channels // ring
    rows = parts * antennas
    hops = ring // 2 + 1
    set_count = tap_table.shape[0]
    out = pl.pallas_call(
        functools.partial(kernel, ring, blocks),
        out_shape=jax.ShapeDtypeStruct((per, 2 * beams, time), BF16),
        in_specs=[
            pl.BlockSpec(memory_space=pltpu.HBM),
            pl.BlockSpec(memory_space=pltpu.HBM),
            pl.BlockSpec(memory_space=pltpu.HBM),
            pl.BlockSpec(memory_space=pltpu.SMEM),
            pl.BlockSpec(memory_space=pltpu.HBM),
        ],
        out_specs=pl.BlockSpec(memory_space=pltpu.VMEM),
        scratch_shapes=[
            pltpu.SMEM(tap_sets.shape, jnp.int32),
            pltpu.VMEM(tap_table.shape, BF16),
            pltpu.VMEM((ring, per, rows, time), BF16),
            pltpu.VMEM((ring, per, rows, beams), BF16),
            pltpu.VMEM((ring, per, RIM, rows), BF16),
            pltpu.VMEM((ring, per, RIM, rows), BF16),
            pltpu.VMEM((set_count, time, time), BF16),
            pltpu.VMEM((set_count, RIM, RIM), BF16),
            pltpu.VMEM((2 * per, RIM, rows), F32),
            pltpu.VMEM((ring, per, time, 2 * beams), F32),
            pltpu.VMEM((2, hops, per, time, 2 * beams), BF16),
            pltpu.VMEM((2, hops, per, time, 2 * beams), BF16),
            pltpu.SemaphoreType.DMA((2,)),
            pltpu.SemaphoreType.DMA((ring, 2)),
            pltpu.SemaphoreType.DMA((ring, 2)),
            pltpu.SemaphoreType.DMA((ring, 2)),
            pltpu.SemaphoreType.DMA((2, hops, per)),
            pltpu.SemaphoreType.DMA((2, hops, per)),
        ],
        compiler_params=pltpu.CompilerParams(
            collective_id=0, has_side_effects=True, vmem_limit_bytes=53 * 1024 * 1024
        ),
    )(
        voltages.reshape(channels, rows, time),
        weights.reshape(channels, rows, beams),
        tap_sets,
        delays,
        tap_table,
    )
    return out.reshape(per, 2, beams, time)


def solution(mesh):
    return jax.shard_map(
        functools.partial(body, mesh.shape["station"], mesh.shape["tm"]),
        mesh=mesh,
        in_specs=(
            P(("group", "station"), "chan", None, None, "tm"),
            P(("group", "station")),
            P(("group", "station"), "chan"),
            P(),
            P(("group", "station"), "chan", None, None, None),
        ),
        out_specs=P(("group", "chan", "station"), None, None, "tm"),
        check_vma=False,
    )
```
